32 devices in a mesh: groups: 2 (over y), tiles: 4 (over z), heads: 2 (over x), kv: 2 (over core).
Axes of the slice: x: 2, y: 2, z: 4, core: 2. Of those that a mesh axis runs over, the one named last changes fastest.
Arguments:
- features: bfloat16 [12288, 1536], P(('groups', 'tiles')), parts along dimension 0, may hold values from -6 to 6
- counts: int32 [8], P(('groups', 'tiles')), parts along dimension 0, may hold values from 1 to 6
- tile_mask: int32 [48, 256], P(('groups', 'tiles')), parts along dimension 0, may hold values from 0 to 1, as said below
- queries: bfloat16 [256, 768], P(('heads', 'kv')), may hold values from -6 to 6
- norm_gain: float32 [2, 768], replicated, may hold values from 0.5 to 1.5
- head_scale: float32 [12], P('heads'), may hold values from 1 to 4
- w_query: bfloat16 [2, 768, 768], P(None, None, ('heads', 'kv')), may hold values from -0.21875 to 0.21875
- w_kv: bfloat16 [2, 1536, 2, 768], P(None, None, 'kv', 'heads'), may hold values from -0.15625 to 0.15625
- w_out: bfloat16 [2, 768, 768], P(None, ('heads', 'kv')), may hold values from -0.21875 to 0.21875
Outputs:
- query_states: float32 [512, 768], P(('groups', 'heads', 'kv')), parts along dimension 0
The draws below stay inside these ranges and needn't reach their ends.
There are 2 independent parts, one for each index of `groups`. The reference program is written for one: setup_inputs(seed, part) draws one part's arguments, and reference() takes and returns one part's arrays. A program takes and returns all parts, laid end to end along the dimension named above; an argument that names none is the same for every part. Nothing has to cross between parts.
Inputs may be any that keep to these rules, and one draw needn't show every extreme that they name: `tile_mask`: the first tile of every block slot is 1.
All inputs are finite; a program needn't handle non-finite values.
Results may differ from the reference program's by a relative error of at most 0.012.
The reference program's roundings to bfloat16 on the way count: a program that leaves them out, or rounds other values in their place, can miss the bound.
Values may be sent and summed in bfloat16 or wider, within the bound.
No kernel may reach another device: no remote copies, remote signals or barrier semaphores. Data moves between devices by JAX's collectives and lax.ppermute only.
A program may use at most 64 MiB of HBM per device.

```python
import math
import jax
import jax.numpy as jnp
from jax import lax

FEAT = 1536
NQ = 256
NH = 12
HD = 64
LAYERS = 2
BLK = 256
SLOTS = 6
DQ = 768
TILES = 6144
N_TILES = 4


def draw_tile_mask(key, part):
    marks = jax.random.randint(jax.random.fold_in(key, 11), (TILES // BLK, BLK), 0, 4)
    filled = (marks > 0).astype(jnp.int32)
    leading = (jnp.arange(BLK, dtype=jnp.int32) == 0)[None, :]
    return jnp.where(leading, 1, filled).astype(jnp.int32)


def place_ends(values, rng, least, top_value):
    place = [jax.random.randint(jax.random.fold_in(rng, axis), (), 0, length) for axis, length in enumerate(values.shape)]
    longest = values.shape.index(max(values.shape))
    neighbour = place[:longest] + [(place[longest] + 1) % values.shape[longest]] + place[longest + 1:]
    return values.at[tuple(place)].set(least).at[tuple(neighbour)].set(top_value)


def block_levels(stream_key, dims, cuts, low, largest):
    def one(position, parts):
        heights = jax.random.uniform(jax.random.fold_in(jax.random.fold_in(stream_key, 6), position), (parts,), jnp.float32, low / len(cuts), largest / len(cuts))
        return jnp.repeat(jnp.exp(heights), dims[position] // parts).reshape((-1,) + (1,) * (len(dims) - position - 1))

    gain = one(*cuts[0])
    for cut in cuts[1:]:
        gain = gain * one(*cut)
    return gain


def gaussian(own_key, extent, scale, limit, shards=(), held_as=jnp.bfloat16):
    level = block_levels(own_key, extent, shards, -0.22, 0.18) if shards else 1.0
    result = jax.random.normal(own_key, extent, jnp.float32) * scale * level
    return jnp.minimum(jnp.maximum(result, -limit), limit).astype(held_as)


def setup_inputs(seed: int = 0, part: int = 0) -> dict:
    seeds = jax.random.split(jax.random.key(seed), 10)
    part_splits = jax.random.split(jax.random.fold_in(seeds[9], part), 10)
    features = gaussian(part_splits[0], (TILES, FEAT), 1.0, 6.0, ((0, 4),))
    counts = place_ends(jax.random.randint(part_splits[1], (N_TILES,), 1, SLOTS + 1), jax.random.fold_in(part_splits[1], 1), 1, SLOTS).astype(jnp.int32)
    tile_mask = draw_tile_mask(jax.random.fold_in(jax.random.fold_in(seeds[9], part), 71), part)
    queries = gaussian(seeds[3], (NQ, DQ), 1.0, 6.0, ((0, 4),))
    norm_gain = jnp.clip(1.0 + 0.1 * jax.random.normal(seeds[4], (LAYERS, DQ), jnp.float32), 0.5, 1.5)
    head_scale = jnp.clip(jnp.exp(math.log(4.0) - 1.3862944 * jax.random.uniform(seeds[5], (NH,), jnp.float32) ** block_levels(seeds[5], (NH,), ((0, 2),), -0.2, 0.2)), 1.0, 4.0)
    w_query = gaussian(seeds[6], (LAYERS, DQ, DQ), DQ ** -0.5, 0.21875, ((2, 4),))
    w_kv = gaussian(seeds[7], (LAYERS, FEAT, 2, DQ), FEAT ** -0.5, 0.15625, ((2, 2), (3, 2)))
    w_out = gaussian(seeds[8], (LAYERS, DQ, DQ), DQ ** -0.5, 0.21875, ((1, 4),))
    return dict(features=features, counts=counts, tile_mask=tile_mask, queries=queries, norm_gain=norm_gain, head_scale=head_scale, w_query=w_query, w_kv=w_kv, w_out=w_out)


SOFT_CAP = 50.0
NORM_EPS = 1e-06

def normalize(hidden, gain_row):
    return hidden * jax.lax.rsqrt(lax.optimization_barrier(jnp.mean(hidden * hidden, axis=-1, keepdims=True)) + NORM_EPS) * gain_row

def reference(features, counts, tile_mask, queries, norm_gain, head_scale, w_query, w_kv, w_out):
    block_ids = jnp.arange(TILES // BLK, dtype=jnp.int32)
    live_slots = (block_ids % SLOTS < jnp.repeat(counts, SLOTS)).astype(jnp.int32)
    valid_tiles = (tile_mask * live_slots[:, None]).reshape(TILES).astype(jnp.float32)
    states = queries.astype(jnp.float32)
    for layer_at in range(LAYERS):
        normed = normalize(states, norm_gain[layer_at]).astype(jnp.bfloat16)
        query_all = jnp.dot(normed, w_query[layer_at], preferred_element_type=jnp.float32).astype(jnp.bfloat16)
        keys = jnp.dot(features, w_kv[layer_at, :, 0, :], preferred_element_type=jnp.float32).astype(jnp.bfloat16)
        values = jnp.dot(features, w_kv[layer_at, :, 1, :], preferred_element_type=jnp.float32).astype(jnp.bfloat16)
        pieces = []
        for head_at in range(NH):
            low = head_at * HD
            scores = jnp.dot(query_all[:, low:low + HD], keys[:, low:low + HD].T, preferred_element_type=jnp.float32)
            scores = scores * (head_scale[head_at] / math.sqrt(HD))
            capped = SOFT_CAP * jnp.tanh(scores / SOFT_CAP)
            weights = jnp.exp(capped) * valid_tiles[None, :]
            totals = lax.optimization_barrier(jnp.sum(weights, axis=1, keepdims=True))
            partial_value = jnp.dot(weights.astype(jnp.bfloat16), values[:, low:low + HD], preferred_element_type=jnp.float32)
            pieces.append(partial_value / totals)
        attended = jnp.concatenate(pieces, axis=1).astype(jnp.bfloat16)
        states = states + jnp.dot(attended, w_out[layer_at], preferred_element_type=jnp.float32)
    return states
```

```python
import functools
import math

import jax
import jax.numpy as jnp
from jax import lax
from jax.experimental import pallas as pl
from jax.experimental.pallas import tpu as pltpu
from jax.sharding import PartitionSpec as P

SOFT_CAP = 50.0
NORM_EPS = 1e-06
LANES = 128
SPLIT = 16


def normalize(hidden, gain_row):
    return (
        hidden * lax.rsqrt(jnp.mean(hidden * hidden, axis=-1, keepdims=True) + NORM_EPS) * gain_row
    )


def generic_body(features, counts, tile_mask, queries, norm_gain, head_scale, w_query, w_kv, w_out):
    slot_count = tile_mask.shape[0]
    block_rows = tile_mask.shape[1]
    total_rows = slot_count * block_rows
    half_rows = total_rows // 2
    layer_count = w_kv.shape[0]
    head_cols = w_kv.shape[3]
    heads_local = head_scale.shape[0]
    head_dim = head_cols // heads_local
    kv_side = lax.axis_index("kv")
    kv_weights = w_kv[:, :, 0, :]
    slot_ids = jnp.arange(slot_count, dtype=jnp.int32)

    def add_block(slot_at, current):
        block_feats = lax.dynamic_slice_in_dim(features, slot_at * block_rows, block_rows, 0)
        result = jnp.einsum(
            "rf,lfc->lrc", block_feats, kv_weights, preferred_element_type=jnp.float32
        )
        return lax.dynamic_update_slice_in_dim(
            current, result.astype(jnp.bfloat16), slot_at * block_rows, 1
        )

    own_count = counts[0]
    projected = jnp.zeros((layer_count, total_rows, head_cols), jnp.bfloat16)
    projected = lax.fori_loop(jnp.int32(0), own_count, add_block, projected)
    live_mask = tile_mask * (slot_ids < own_count).astype(jnp.int32)[:, None]
    kv_local = lax.all_to_all(projected, "kv", split_axis=1, concat_axis=2, tiled=True)
    valid_tiles = lax.dynamic_slice_in_dim(
        live_mask.reshape(total_rows).astype(jnp.float32), kv_side * half_rows, half_rows, 0
    )
    states = queries.astype(jnp.float32)
    scale_vec = head_scale / math.sqrt(head_dim)
    for layer_at in range(layer_count):
        normed = lax.all_gather(
            normalize(states, norm_gain[layer_at]).astype(jnp.bfloat16),
            ("heads", "kv"),
            axis=0,
            tiled=True,
        )
        query_part = jnp.dot(normed, w_query[layer_at], preferred_element_type=jnp.float32).astype(
            jnp.bfloat16
        )
        query_cols = lax.all_gather(query_part, "kv", axis=1, tiled=True)
        n_queries = query_cols.shape[0]
        query_heads = query_cols.reshape(n_queries, heads_local, head_dim)
        key_heads = kv_local[layer_at, :, :head_cols].reshape(half_rows, heads_local, head_dim)
        value_heads = kv_local[layer_at, :, head_cols:].reshape(half_rows, heads_local, head_dim)
        scores = jnp.einsum(
            "qhd,khd->hqk", query_heads, key_heads, preferred_element_type=jnp.float32
        )
        scores = scores * scale_vec[:, None, None]
        capped = SOFT_CAP * jnp.tanh(scores / SOFT_CAP)
        weights_p = jnp.exp(capped) * valid_tiles[None, None, :]
        totals = jnp.sum(weights_p, axis=2)
        partial_value = jnp.einsum(
            "hqk,khd->qhd",
            weights_p.astype(jnp.bfloat16),
            value_heads,
            preferred_element_type=jnp.float32,
        )
        totals, partial_value = lax.psum((totals, partial_value), ("tiles", "kv"))
        attended = (
            (partial_value / jnp.transpose(totals)[:, :, None])
            .reshape(n_queries, head_cols)
            .astype(jnp.bfloat16)
        )
        own_cols = lax.dynamic_slice_in_dim(attended, kv_side * (head_cols // 2), head_cols // 2, 1)
        states = states + lax.psum_scatter(
            jnp.dot(own_cols, w_out[layer_at], preferred_element_type=jnp.float32),
            ("heads", "kv"),
            scatter_dimension=0,
            tiled=True,
        )
    return states


class Plan:
    def __init__(self, mesh, queries, head_scale, w_kv):
        self.n_t, self.n_h, self.n_k = (mesh.shape[a] for a in ("tiles", "heads", "kv"))
        self.q_rows, self.dq = queries.shape
        self.n_q = self.q_rows * self.n_h * self.n_k
        self.cols = w_kv.shape[3]
        self.heads = head_scale.shape[0] // self.n_k
        self.head_dim = self.cols // head_scale.shape[0]
        self.half = self.heads * self.head_dim
        self.width = -(-self.half // LANES) * LANES
        self.start = [k * self.half // LANES * LANES for k in range(self.n_k)]
        self.off = [k * self.half - s for k, s in enumerate(self.start)]
        offsets = [(t, h) for t in range(self.n_t) for h in range(self.n_h)][1:]
        offsets = sorted(offsets, reverse=True)
        offsets += [None] * (-len(offsets) % self.n_k)
        self.rounds = [
            tuple(offsets[i + k] for k in range(self.n_k))
            for i in range(0, len(offsets), self.n_k)
        ]

    def usable(self):
        return (
            self.n_k == 2
            and self.n_h == 2
            and self.n_t == self.n_h * self.n_k
            and self.half * self.n_k == self.cols
            and self.cols % LANES == 0
            and self.q_rows % 16 == 0
            and self.off[0] == 0
            and all(s + self.width <= self.cols for s in self.start)
            and all(o == 0 or o + self.half == self.width for o in self.off)
            and self.width - self.half >= 2 * SPLIT
            and self.heads <= SPLIT
        )


def place():
    return lax.axis_index("tiles"), lax.axis_index("heads"), lax.axis_index("kv")


def rows_at(index, size):
    return pl.ds(pl.multiple_of(index * size, size), size)


def project_kernel(plan, count_ref, mask_ref, feats_ref, weights_ref, own_ref, other_ref):
    side = lax.axis_index("kv")
    slot = pl.program_id(0)
    acc = jnp.dot(feats_ref[...], weights_ref[0], preferred_element_type=jnp.float32)
    rows = acc.shape[0]
    marks = mask_ref[pl.ds(slot, 1), :].astype(jnp.float32)
    marks = jnp.where(slot < count_ref[0], marks, 0.0)
    valid = jnp.broadcast_to(marks, (LANES, rows)).T
    valid = jnp.concatenate([valid] * (plan.width // LANES), axis=1)
    lane = lax.broadcasted_iota(jnp.int32, (1, plan.width), 1)
    pieces = []
    for start, off in zip(plan.start, plan.off):
        inside = (lane >= off) & (lane < off + plan.half)
        block = acc[:, start : start + plan.width]
        pieces.append(jnp.where(inside, block * valid, valid).astype(jnp.bfloat16))
    own_ref[...] = jnp.where(side == 0, pieces[0], pieces[1])
    other_ref[...] = jnp.where(side == 0, pieces[1], pieces[0])


def project(plan, layer, counts, tile_mask, features, weights):
    slots, rows = tile_mask.shape
    feat = features.shape[1]
    out = jax.ShapeDtypeStruct((slots * rows, plan.width), jnp.bfloat16)
    out_spec = pl.BlockSpec((rows, plan.width), lambda i: (i, 0))
    return pl.pallas_call(
        functools.partial(project_kernel, plan),
        grid=(slots,),
        out_shape=(out, out),
        in_specs=[
            pl.BlockSpec(memory_space=pltpu.SMEM),
            pl.BlockSpec((slots, rows), lambda i: (0, 0)),
            pl.BlockSpec((rows, feat), lambda i: (i, 0)),
            pl.BlockSpec((1, feat, plan.cols), lambda i: (layer, 0, 0)),
        ],
        out_specs=(out_spec, out_spec),
        cost_estimate=pl.CostEstimate(
            flops=2 * slots * rows * feat * plan.cols,
            bytes_accessed=2 * feat * (slots * rows + plan.cols),
            transcendentals=0,
        ),
        name="project",
    )(counts, tile_mask, features, weights)


def attend(plan, query, scale_ref, own_ref, recv_ref, chunk_refs, mix):
    me_t, _, side = place()
    first = side == 0
    off = jnp.where(first, plan.off[0], plan.off[1])
    pad = jnp.where(first, plan.half if plan.off[0] == 0 else 0, plan.half if plan.off[1] == 0 else 0)
    lane = lax.broadcasted_iota(jnp.int32, (1, plan.width), 1)
    factor = SOFT_CAP * math.log2(math.e)
    n_keys = own_ref.shape[0]
    block = min(n_keys, 512)
    masked, scales, totals = [], [], []
    for head in range(plan.heads):
        low = off + head * plan.head_dim
        masked.append(
            jnp.where((lane >= low) & (lane < low + plan.head_dim), query, jnp.zeros_like(query))
        )
        scales.append(
            scale_ref[side * plan.heads + head] * (1.0 / (SOFT_CAP * math.sqrt(plan.head_dim)))
        )
        totals.append(None)
    for at in range(0, n_keys, block):
        mine = own_ref[at : at + block, :]
        theirs = recv_ref[at : at + block, :]
        keys = jnp.where(first, mine, theirs)
        values = jnp.where(first, theirs, mine)
        for head in range(plan.heads):
            scores = lax.dot_general(
                masked[head], keys, (((1,), (1,)), ((), ())), preferred_element_type=jnp.float32
            )
            weight = jnp.exp2(jnp.tanh(scores * scales[head]) * factor)
            part = jnp.dot(
                weight.astype(jnp.bfloat16), values, preferred_element_type=jnp.float32
            )
            totals[head] = part if totals[head] is None else totals[head] + part
    result = jnp.zeros((plan.n_q, plan.width), jnp.float32)
    spot = lane - pad
    spare = (spot >= 0) & (spot < 2 * SPLIT)
    for head in range(plan.heads):
        low = off + head * plan.head_dim
        keep = (lane >= low) & (lane < low + plan.head_dim)
        keep = keep | (spare & (jnp.bitwise_and(spot, SPLIT - 1) == head))
        result = jnp.where(keep, totals[head], result)
    rounded = result.astype(jnp.bfloat16).astype(jnp.float32)
    late = spare & (spot >= SPLIT)
    mix[...] = jnp.where(late, result - rounded, rounded)
    for index, ref in enumerate(chunk_refs):
        rows = plan.n_q // plan.n_t
        ref[...] = mix[rows_at(jnp.bitwise_xor(me_t, index), rows), :].astype(ref.dtype)


def query_of(plan, states, gain, wq_ref, wq_pad):
    side = lax.axis_index("kv")
    mean = jnp.mean(states * states, axis=-1, keepdims=True)
    normed = (states * lax.rsqrt(mean + NORM_EPS) * gain).astype(jnp.bfloat16)
    wq_pad[...] = jnp.zeros_like(wq_pad)
    step = max(plan.off)
    wq_pad[pl.ds(pl.multiple_of(side * step, step), plan.half), :] = wq_ref[0]
    return lax.dot_general(
        normed, wq_pad[...], (((1,), (1,)), ((), ())), preferred_element_type=jnp.float32
    ).astype(jnp.bfloat16)


def first_kernel(
    plan, scale_ref, q_ref, qk_ref, qx_ref, qxk_ref, gain_ref, wq_ref, own_ref, recv_ref, *rest
):
    chunks, (all_ref, wq_pad, mix) = rest[: plan.n_t], rest[plan.n_t :]
    _, me_h, me_k = place()
    for dh, row in enumerate(((q_ref, qk_ref), (qx_ref, qxk_ref))):
        for dk, ref in enumerate(row):
            index = jnp.bitwise_xor(me_h, dh) * plan.n_k + jnp.bitwise_xor(me_k, dk)
            all_ref[rows_at(index, plan.q_rows), :] = ref[...]
    states = all_ref[...].astype(jnp.float32)
    query = query_of(plan, states, gain_ref[0:1, :], wq_ref, wq_pad)
    attend(plan, query, scale_ref, own_ref, recv_ref, chunks, mix)


def fill_out(plan, wo_refs, wo_all):
    me_k = lax.axis_index("kv")
    for dh in range(plan.n_h):
        for dk in range(plan.n_k):
            index = dh * plan.n_k + jnp.bitwise_xor(me_k, dk)
            wo_all[rows_at(index, plan.half), :] = wo_refs[dh * plan.n_k + dk][0]


def layer_kernel(
    plan,
    layer,
    scale_ref,
    all_ref,
    block_ref,
    near_ref,
    far_ref,
    wo0,
    wo1,
    wo2,
    wo3,
    gain_ref,
    wq_ref,
    own_ref,
    recv_ref,
    *rest,
):
    chunks, (kept_ref, att, wo_all, states_ref, wq_pad, mix) = rest[: plan.n_t], rest[plan.n_t :]
    me_t, me_h, me_k = place()
    rows = plan.n_q // plan.n_t
    fill_out(plan, (wo0, wo1, wo2, wo3), wo_all)
    for index, pair in enumerate(plan.rounds):
        for ref, flip in ((near_ref, 0), (far_ref, 1)):
            choice = [pair[k ^ flip] or (0, 0) for k in range(2)]
            dt = jnp.where(me_k == 0, choice[0][0], choice[1][0])
            dh = jnp.where(me_k == 0, choice[0][1], choice[1][1])
            att[dh, rows_at(jnp.bitwise_xor(me_t, dt), rows), :] = ref[
                index * rows : index * rows + rows, :
            ]
    att[0, rows_at(me_t, rows), :] = block_ref[...]
    out = jnp.dot(att[0], wo_all[: plan.cols, :], preferred_element_type=jnp.float32)
    out = out + jnp.dot(att[1], wo_all[plan.cols :, :], preferred_element_type=jnp.float32)
    states = all_ref[...].astype(jnp.float32) + out
    states_ref[...] = states
    kept_ref[...] = states_ref[rows_at(me_h * plan.n_k + me_k, plan.q_rows), :]
    query = query_of(plan, states, gain_ref[layer : layer + 1, :], wq_ref, wq_pad)
    attend(plan, query, scale_ref, own_ref, recv_ref, chunks, mix)


def last_kernel(plan, kept_ref, near_ref, far_ref, wo0, wo1, wo2, wo3, out_ref, att, wo_all):
    me_t = lax.axis_index("tiles")
    fill_out(plan, (wo0, wo1, wo2, wo3), wo_all)
    for index, ref in enumerate((near_ref, far_ref)):
        att[(me_t + index) % plan.n_h] = ref[...]
    out = jnp.dot(att[0], wo_all[: plan.cols, :], preferred_element_type=jnp.float32)
    out = out + jnp.dot(att[1], wo_all[plan.cols :, :], preferred_element_type=jnp.float32)
    out_ref[...] = kept_ref[...] + out


def combine_kernel(plan, *refs):
    *parts, out_ref = refs
    side = lax.axis_index("kv")
    first = side == 0
    off = jnp.where(first, plan.off[0], plan.off[1])
    pad = jnp.where(first, plan.half if plan.off[0] == 0 else 0, plan.half if plan.off[1] == 0 else 0)
    lane = lax.broadcasted_iota(jnp.int32, (1, plan.width), 1)
    spot = lane - pad
    spare = (spot >= 0) & (spot < 2 * SPLIT)
    total = sum(ref[...].astype(jnp.float32) for ref in parts)
    below = jnp.ones_like(total)
    for head in range(plan.heads):
        low = off + head * plan.head_dim
        mine = spare & (jnp.bitwise_and(spot, SPLIT - 1) == head)
        weight = jnp.sum(jnp.where(mine, total, 0.0), axis=1, keepdims=True)
        below = jnp.where((lane >= low) & (lane < low + plan.head_dim), weight, below)
    out_ref[...] = (total / below).astype(jnp.bfloat16)


def vmem_call(kernel, out_shape, inputs, smem, scratch, name, flops=0):
    specs = [pl.BlockSpec(memory_space=pltpu.SMEM)] * smem
    specs += [s for _, s in inputs[smem:]]
    return pl.pallas_call(
        kernel,
        out_shape=out_shape,
        grid=(1,),
        in_specs=specs,
        out_specs=jax.tree.map(lambda o: whole(o.shape), out_shape),
        scratch_shapes=scratch,
        cost_estimate=pl.CostEstimate(flops=flops, bytes_accessed=1 << 20, transcendentals=0),
        name=name,
    )(*[a for a, _ in inputs])


def whole(shape):
    return pl.BlockSpec(shape, lambda i: (0,) * len(shape))


def one_of(shape, layer):
    return pl.BlockSpec((1, *shape[1:]), lambda i: (layer,) + (0,) * (len(shape) - 1))


def fast_body(plan, features, counts, tile_mask, queries, norm_gain, head_scale, w_query, w_kv, w_out):
    layer_count = w_kv.shape[0]
    rows = plan.n_q // plan.n_t
    axes = ("tiles", "heads", "kv")
    devices = [
        (t, h, k) for t in range(plan.n_t) for h in range(plan.n_h) for k in range(plan.n_k)
    ]
    side = lax.axis_index("kv")

    def number(t, h, k):
        return (t * plan.n_h + h) * plan.n_k + k

    def swap(value, axis):
        size = {"heads": plan.n_h, "kv": plan.n_k}[axis]
        return lax.ppermute(value, axis, [(i, i ^ 1) for i in range(size)])

    def exchange(chunks):
        received = [
            lax.ppermute(chunks[d], "tiles", [(i, i ^ d) for i in range(plan.n_t)])
            for d in range(plan.n_t - 1, 0, -1)
        ]
        shape = jax.ShapeDtypeStruct((rows, plan.width), jnp.bfloat16)
        parts = [(a, whole(a.shape)) for a in [chunks[0], *received]]
        attended = vmem_call(
            functools.partial(combine_kernel, plan), shape, parts, 0, [], "combine"
        )
        partner = swap(attended, "kv")
        low = jnp.where(side == 0, attended, partner)
        high = jnp.where(side == 0, partner, attended)
        lead = plan.start[1]
        overlap = jnp.where(
            lax.broadcasted_iota(jnp.int32, (1, plan.width - lead), 1) < plan.half - lead,
            low[:, lead:],
            high[:, : plan.width - lead],
        )
        return jnp.concatenate([low[:, :lead], overlap, high[:, plan.width - lead :]], axis=1)

    def spread(block):
        received = []
        for pair in plan.rounds:
            links = [
                (number(t, h, k), number(t ^ pair[k][0], h ^ pair[k][1], k))
                for t, h, k in devices
                if pair[k] is not None
            ]
            received.append(lax.ppermute(block, axes, links))
        near = jnp.concatenate(received, axis=0)
        return near, swap(near, "kv")

    def collect(block):
        received = []
        for turn in range(plan.n_h):
            links = []
            for t, h, k in devices:
                source_t, source_h = h * plan.n_k + k, h ^ ((turn + t) % plan.n_h)
                links.append((number(source_t, source_h, (t // plan.n_h) % plan.n_k), number(t, h, k)))
            received.append(lax.ppermute(block, axes, links))
        return received

    weights = w_kv.reshape(layer_count, w_kv.shape[1], plan.cols)
    wq = jnp.swapaxes(w_query, 1, 2)
    q_x = swap(queries, "heads")
    q_k = swap(queries, "kv")
    q_xk = swap(q_x, "kv")
    tied, _ = lax.optimization_barrier((w_out, q_x))
    wo_x = swap(tied, "heads")
    wo = [tied, swap(tied, "kv"), wo_x, swap(wo_x, "kv")]
    pairs = []
    for layer in range(layer_count):
        own, other = project(plan, layer, counts, tile_mask, features, weights)
        pairs.append((own, swap(other, "kv")))

    bf16, f32 = jnp.bfloat16, jnp.float32
    chunk_shapes = [jax.ShapeDtypeStruct((rows, plan.width), f32)]
    chunk_shapes += [jax.ShapeDtypeStruct((rows, plan.width), bf16)] * (plan.n_t - 1)
    wq_scratch = pltpu.VMEM((plan.width, plan.dq), bf16)
    mix_scratch = pltpu.VMEM((plan.n_q, plan.width), f32)
    wo_scratch = pltpu.VMEM((plan.n_h * plan.cols, plan.dq), bf16)

    def plain(*arrays):
        return [(a, whole(a.shape)) for a in arrays]

    outs = vmem_call(
        functools.partial(first_kernel, plan),
        chunk_shapes + [jax.ShapeDtypeStruct((plan.n_q, plan.dq), bf16)],
        plain(head_scale, queries, q_k, q_x, q_xk, norm_gain)
        + [(wq, one_of(wq.shape, 0))]
        + plain(*pairs[0]),
        1,
        [wq_scratch, mix_scratch],
        "first",
        4 * plan.n_q * pairs[0][0].shape[0] * plan.width,
    )
    chunks, states = outs[: plan.n_t], outs[plan.n_t]
    for layer in range(1, layer_count):
        block = exchange(chunks)
        near, far = spread(block)
        outs = vmem_call(
            functools.partial(layer_kernel, plan, layer),
            chunk_shapes + [jax.ShapeDtypeStruct((plan.q_rows, plan.dq), f32)],
            plain(head_scale, states, block, near, far)
            + [(w, one_of(w.shape, layer - 1)) for w in wo]
            + plain(norm_gain)
            + [(wq, one_of(wq.shape, layer))]
            + plain(*pairs[layer]),
            1,
            [
                pltpu.VMEM((plan.n_h, plan.n_q, plan.cols), bf16),
                wo_scratch,
                pltpu.VMEM((plan.n_q, plan.dq), f32),
                wq_scratch,
                mix_scratch,
            ],
            "layer",
            4 * plan.n_q * pairs[0][0].shape[0] * plan.width,
        )
        chunks, kept = outs[: plan.n_t], outs[plan.n_t]
    block = exchange(chunks)
    near, far = collect(block)
    return vmem_call(
        functools.partial(last_kernel, plan),
        jax.ShapeDtypeStruct((plan.q_rows, plan.dq), f32),
        plain(kept, near, far) + [(w, one_of(w.shape, layer_count - 1)) for w in wo],
        0,
        [pltpu.VMEM((plan.n_h, plan.q_rows, plan.cols), bf16), wo_scratch],
        "last",
    )


def solution(mesh):
    def body(features, counts, tile_mask, queries, norm_gain, head_scale, w_query, w_kv, w_out):
        args = (features, counts, tile_mask, queries, norm_gain, head_scale, w_query, w_kv, w_out)
        plan = Plan(mesh, queries, head_scale, w_kv)
        if w_kv.shape[0] == 2 and plan.usable():
            return fast_body(plan, *args)
        return generic_body(*args)

    return jax.shard_map(
        body,
        mesh=mesh,
        in_specs=(
            P(("groups", "tiles"), None),
            P(("groups", "tiles")),
            P(("groups", "tiles"), None),
            P(("heads", "kv"), None),
            P(),
            P("heads"),
            P(None, None, ("heads", "kv")),
            P(None, None, "kv", "heads"),
            P(None, ("heads", "kv"), None),
        ),
        out_specs=P(("groups", "heads", "kv"), None),
        check_vma=False,
    )
```

```python
import functools
import math

import jax
import jax.numpy as jnp
from jax import lax
from jax.experimental import pallas as pl
from jax.experimental.pallas import tpu as pltpu
from jax.sharding import PartitionSpec as P


SOFT_CAP = 50.0
NORM_EPS = 1e-06
LANES = 128
SPLIT = 16
ROOM = 4 << 20


def normalize(hidden, gain_row):
    return (
        hidden * lax.rsqrt(jnp.mean(hidden * hidden, axis=-1, keepdims=True) + NORM_EPS) * gain_row
    )


def generic_body(features, counts, tile_mask, queries, norm_gain, head_scale, w_query, w_kv, w_out):
    slot_count = tile_mask.shape[0]
    block_rows = tile_mask.shape[1]
    total_rows = slot_count * block_rows
    half_rows = total_rows // 2
    layer_count = w_kv.shape[0]
    head_cols = w_kv.shape[3]
    heads_local = head_scale.shape[0]
    head_dim = head_cols // heads_local
    kv_side = lax.axis_index("kv")
    kv_weights = w_kv[:, :, 0, :]
    slot_ids = jnp.arange(slot_count, dtype=jnp.int32)

    def add_block(slot_at, current):
        block_feats = lax.dynamic_slice_in_dim(features, slot_at * block_rows, block_rows, 0)
        result = jnp.einsum(
            "rf,lfc->lrc", block_feats, kv_weights, preferred_element_type=jnp.float32
        )
        return lax.dynamic_update_slice_in_dim(
            current, result.astype(jnp.bfloat16), slot_at * block_rows, 1
        )

    own_count = counts[0]
    projected = jnp.zeros((layer_count, total_rows, head_cols), jnp.bfloat16)
    projected = lax.fori_loop(jnp.int32(0), own_count, add_block, projected)
    live_mask = tile_mask * (slot_ids < own_count).astype(jnp.int32)[:, None]
    kv_local = lax.all_to_all(projected, "kv", split_axis=1, concat_axis=2, tiled=True)
    valid_tiles = lax.dynamic_slice_in_dim(
        live_mask.reshape(total_rows).astype(jnp.float32), kv_side * half_rows, half_rows, 0
    )
    states = queries.astype(jnp.float32)
    scale_vec = head_scale / math.sqrt(head_dim)
    for layer_at in range(layer_count):
        normed = lax.all_gather(
            normalize(states, norm_gain[layer_at]).astype(jnp.bfloat16),
            ("heads", "kv"),
            axis=0,
            tiled=True,
        )
        query_part = jnp.dot(normed, w_query[layer_at], preferred_element_type=jnp.float32).astype(
            jnp.bfloat16
        )
        query_cols = lax.all_gather(query_part, "kv", axis=1, tiled=True)
        n_queries = query_cols.shape[0]
        query_heads = query_cols.reshape(n_queries, heads_local, head_dim)
        key_heads = kv_local[layer_at, :, :head_cols].reshape(half_rows, heads_local, head_dim)
        value_heads = kv_local[layer_at, :, head_cols:].reshape(half_rows, heads_local, head_dim)
        scores = jnp.einsum(
            "qhd,khd->hqk", query_heads, key_heads, preferred_element_type=jnp.float32
        )
        scores = scores * scale_vec[:, None, None]
        capped = SOFT_CAP * jnp.tanh(scores / SOFT_CAP)
        weights_p = jnp.exp(capped) * valid_tiles[None, None, :]
        totals = jnp.sum(weights_p, axis=2)
        partial_value = jnp.einsum(
            "hqk,khd->qhd",
            weights_p.astype(jnp.bfloat16),
            value_heads,
            preferred_element_type=jnp.float32,
        )
        totals, partial_value = lax.psum((totals, partial_value), ("tiles", "kv"))
        attended = (
            (partial_value / jnp.transpose(totals)[:, :, None])
            .reshape(n_queries, head_cols)
            .astype(jnp.bfloat16)
        )
        own_cols = lax.dynamic_slice_in_dim(attended, kv_side * (head_cols // 2), head_cols // 2, 1)
        states = states + lax.psum_scatter(
            jnp.dot(own_cols, w_out[layer_at], preferred_element_type=jnp.float32),
            ("heads", "kv"),
            scatter_dimension=0,
            tiled=True,
        )
    return states


class Plan:
    def __init__(self, mesh, queries, head_scale, w_kv):
        self.n_t, self.n_h, self.n_k = (mesh.shape[a] for a in ("tiles", "heads", "kv"))
        self.q_rows, self.dq = queries.shape
        self.n_q = self.q_rows * self.n_h * self.n_k
        self.cols = w_kv.shape[3]
        self.heads = head_scale.shape[0] // self.n_k
        self.head_dim = self.cols // head_scale.shape[0]
        self.half = self.heads * self.head_dim
        self.width = -(-self.half // LANES) * LANES
        self.start = [k * self.half // LANES * LANES for k in range(self.n_k)]
        self.off = [k * self.half - s for k, s in enumerate(self.start)]
        offsets = [(t, h) for t in range(self.n_t) for h in range(self.n_h)][1:]
        offsets = sorted(offsets, reverse=True)
        offsets += [None] * (-len(offsets) % self.n_k)
        self.rounds = [
            tuple(offsets[i + k] for k in range(self.n_k))
            for i in range(0, len(offsets), self.n_k)
        ]

    def usable(self):
        return (
            self.n_k == 2
            and self.n_h == 2
            and self.n_t == self.n_h * self.n_k
            and self.half * self.n_k == self.cols
            and self.cols % LANES == 0
            and self.q_rows % 16 == 0
            and self.off[0] == 0
            and all(s + self.width <= self.cols for s in self.start)
            and all(o == 0 or o + self.half == self.width for o in self.off)
            and self.width - self.half >= 2 * SPLIT
            and self.heads <= SPLIT
        )


def place():
    return lax.axis_index("tiles"), lax.axis_index("heads"), lax.axis_index("kv")


def rows_at(index, size):
    return pl.ds(pl.multiple_of(index * size, size), size)


def project_rows(plan, count_ref, mask_ref, feats, weights, own_ref, other_ref, low, high):
    first = lax.axis_index("kv") == 0
    rows = mask_ref.shape[1]
    lane = lax.broadcasted_iota(jnp.int32, (1, plan.width), 1)
    acc = jnp.dot(feats[low:high, :], weights[...], preferred_element_type=jnp.float32)
    for slot in range(low // rows, high // rows):
        marks = mask_ref[slot : slot + 1, :].astype(jnp.float32)
        marks = jnp.where(slot < count_ref[0], marks, 0.0)
        valid = jnp.broadcast_to(marks, (LANES, rows)).T
        valid = jnp.concatenate([valid] * (plan.width // LANES), axis=1)
        part = acc[slot * rows - low : slot * rows - low + rows]
        pieces = []
        for start, off in zip(plan.start, plan.off):
            inside = (lane >= off) & (lane < off + plan.half)
            block = part[:, start : start + plan.width]
            pieces.append(jnp.where(inside, block * valid, valid).astype(jnp.bfloat16))
        at = slice(slot * rows, slot * rows + rows)
        own_ref[at, :] = jnp.where(first, pieces[0], pieces[1])
        other_ref[at, :] = jnp.where(first, pieces[1], pieces[0])


def group_of(mask_ref):
    slots, rows = mask_ref.shape
    return rows * (2 if slots % 2 == 0 else 1)


def load_project_kernel(
    plan,
    count_ref,
    mask_ref,
    feats_hbm,
    weights_hbm,
    own_ref,
    other_ref,
    feats_ref,
    later_ref,
    weights_ref,
    sems,
):
    size = group_of(mask_ref)
    groups = feats_ref.shape[0] // size
    copies = [pltpu.make_async_copy(weights_hbm.at[0], weights_ref, sems.at[groups])]
    for index in range(groups):
        at = pl.ds(index * size, size)
        copies.append(
            pltpu.make_async_copy(feats_hbm.at[at], feats_ref.at[at], sems.at[index])
        )
    copies.append(pltpu.make_async_copy(weights_hbm.at[1], later_ref, sems.at[groups + 1]))
    for copy in copies:
        copy.start()
    copies[0].wait()
    for index in range(groups):
        copies[1 + index].wait()
        low = index * size
        project_rows(
            plan, count_ref, mask_ref, feats_ref, weights_ref, own_ref, other_ref, low, low + size
        )
    copies[-1].wait()


def project_kernel(plan, count_ref, mask_ref, feats_ref, weights_ref, own_ref, other_ref):
    size = group_of(mask_ref)
    for low in range(0, feats_ref.shape[0], size):
        project_rows(
            plan, count_ref, mask_ref, feats_ref, weights_ref, own_ref, other_ref, low, low + size
        )


def attend(plan, query, scale_ref, own_ref, recv_ref, chunk_refs, mix):
    me_t, _, side = place()
    first = side == 0
    off = jnp.where(first, plan.off[0], plan.off[1])
    pad = jnp.where(first, plan.half if plan.off[0] == 0 else 0, plan.half if plan.off[1] == 0 else 0)
    lane = lax.broadcasted_iota(jnp.int32, (1, plan.width), 1)
    factor = SOFT_CAP * math.log2(math.e)
    n_keys = own_ref.shape[0]
    block = min(n_keys, 512)
    masked, scales, totals = [], [], []
    for head in range(plan.heads):
        low = off + head * plan.head_dim
        masked.append(
            jnp.where((lane >= low) & (lane < low + plan.head_dim), query, jnp.zeros_like(query))
        )
        scales.append(
            scale_ref[side * plan.heads + head] * (1.0 / (SOFT_CAP * math.sqrt(plan.head_dim)))
        )
        totals.append(None)
    for at in range(0, n_keys, block):
        mine = own_ref[at : at + block, :]
        theirs = recv_ref[at : at + block, :]
        keys = jnp.where(first, mine, theirs)
        values = jnp.where(first, theirs, mine)
        for head in range(plan.heads):
            scores = lax.dot_general(
                masked[head], keys, (((1,), (1,)), ((), ())), preferred_element_type=jnp.float32
            )
            weight = jnp.exp2(jnp.tanh(scores * scales[head]) * factor)
            part = jnp.dot(
                weight.astype(jnp.bfloat16), values, preferred_element_type=jnp.float32
            )
            totals[head] = part if totals[head] is None else totals[head] + part
    result = jnp.zeros((plan.n_q, plan.width), jnp.float32)
    spot = lane - pad
    spare = (spot >= 0) & (spot < 2 * SPLIT)
    for head in range(plan.heads):
        low = off + head * plan.head_dim
        keep = (lane >= low) & (lane < low + plan.head_dim)
        keep = keep | (spare & (jnp.bitwise_and(spot, SPLIT - 1) == head))
        result = jnp.where(keep, totals[head], result)
    rounded = result.astype(jnp.bfloat16).astype(jnp.float32)
    late = spare & (spot >= SPLIT)
    mix[...] = jnp.where(late, result - rounded, rounded)
    for index, ref in enumerate(chunk_refs):
        rows = plan.n_q // plan.n_t
        ref[...] = mix[rows_at(jnp.bitwise_xor(me_t, index), rows), :].astype(ref.dtype)


def query_of(plan, states, gain, wq, wq_pad):
    side = lax.axis_index("kv")
    mean = jnp.mean(states * states, axis=-1, keepdims=True)
    normed = (states * lax.rsqrt(mean + NORM_EPS) * gain).astype(jnp.bfloat16)
    wq_pad[...] = jnp.zeros_like(wq_pad)
    step = max(plan.off)
    wq_pad[pl.ds(pl.multiple_of(side * step, step), plan.half), :] = wq
    return lax.dot_general(
        normed, wq_pad[...], (((1,), (1,)), ((), ())), preferred_element_type=jnp.float32
    ).astype(jnp.bfloat16)


def first_kernel(
    plan, scale_ref, q_ref, qk_ref, qx_ref, qxk_ref, gain_ref, wq_ref, own_ref, recv_ref, *rest
):
    chunks, (all_ref, wq_pad, mix) = rest[: plan.n_t], rest[plan.n_t :]
    _, me_h, me_k = place()
    for dh, row in enumerate(((q_ref, qk_ref), (qx_ref, qxk_ref))):
        for dk, ref in enumerate(row):
            index = jnp.bitwise_xor(me_h, dh) * plan.n_k + jnp.bitwise_xor(me_k, dk)
            all_ref[rows_at(index, plan.q_rows), :] = ref[...]
    states = all_ref[...].astype(jnp.float32)
    query = query_of(plan, states, gain_ref[0:1, :], wq_ref[0], wq_pad)
    attend(plan, query, scale_ref, own_ref, recv_ref, chunks, mix)


def fill_out(plan, layer, wo_refs, wo_all):
    me_k = lax.axis_index("kv")
    for dh in range(plan.n_h):
        for dk in range(plan.n_k):
            index = dh * plan.n_k + jnp.bitwise_xor(me_k, dk)
            wo_all[rows_at(index, plan.half), :] = wo_refs[dh * plan.n_k + dk][layer]


def layer_kernel(
    plan,
    layer,
    scale_ref,
    all_ref,
    block_ref,
    near_ref,
    far_ref,
    wo0,
    wo1,
    wo2,
    wo3,
    gain_ref,
    wq_ref,
    own_ref,
    recv_ref,
    *rest,
):
    chunks, (kept_ref, att, wo_all, states_ref, wq_pad, mix) = rest[: plan.n_t], rest[plan.n_t :]
    me_t, me_h, me_k = place()
    rows = plan.n_q // plan.n_t
    fill_out(plan, layer - 1, (wo0, wo1, wo2, wo3), wo_all)
    for index, pair in enumerate(plan.rounds):
        for ref, flip in ((near_ref, 0), (far_ref, 1)):
            choice = [pair[k ^ flip] or (0, 0) for k in range(2)]
            dt = jnp.where(me_k == 0, choice[0][0], choice[1][0])
            dh = jnp.where(me_k == 0, choice[0][1], choice[1][1])
            att[dh, rows_at(jnp.bitwise_xor(me_t, dt), rows), :] = ref[
                index * rows : index * rows + rows, :
            ]
    att[0, rows_at(me_t, rows), :] = block_ref[...]
    out = jnp.dot(att[0], wo_all[: plan.cols, :], preferred_element_type=jnp.float32)
    out = out + jnp.dot(att[1], wo_all[plan.cols :, :], preferred_element_type=jnp.float32)
    states = all_ref[...].astype(jnp.float32) + out
    states_ref[...] = states
    kept_ref[...] = states_ref[rows_at(me_h * plan.n_k + me_k, plan.q_rows), :]
    query = query_of(plan, states, gain_ref[layer : layer + 1, :], wq_ref[layer], wq_pad)
    attend(plan, query, scale_ref, own_ref, recv_ref, chunks, mix)


def last_kernel(plan, layer, kept_ref, near_ref, far_ref, wo0, wo1, wo2, wo3, out_ref, att, wo_all):
    me_t = lax.axis_index("tiles")
    fill_out(plan, layer, (wo0, wo1, wo2, wo3), wo_all)
    for index, ref in enumerate((near_ref, far_ref)):
        att[(me_t + index) % plan.n_h] = ref[...]
    out = jnp.dot(att[0], wo_all[: plan.cols, :], preferred_element_type=jnp.float32)
    out = out + jnp.dot(att[1], wo_all[plan.cols :, :], preferred_element_type=jnp.float32)
    out_ref[...] = kept_ref[...] + out


def combine_kernel(plan, *refs):
    *parts, out_ref = refs
    side = lax.axis_index("kv")
    first = side == 0
    off = jnp.where(first, plan.off[0], plan.off[1])
    pad = jnp.where(first, plan.half if plan.off[0] == 0 else 0, plan.half if plan.off[1] == 0 else 0)
    lane = lax.broadcasted_iota(jnp.int32, (1, plan.width), 1)
    spot = lane - pad
    spare = (spot >= 0) & (spot < 2 * SPLIT)
    total = sum(ref[...].astype(jnp.float32) for ref in parts)
    below = jnp.ones_like(total)
    for head in range(plan.heads):
        low = off + head * plan.head_dim
        mine = spare & (jnp.bitwise_and(spot, SPLIT - 1) == head)
        weight = jnp.sum(jnp.where(mine, total, 0.0), axis=1, keepdims=True)
        below = jnp.where((lane >= low) & (lane < low + plan.head_dim), weight, below)
    out_ref[...] = (total / below).astype(jnp.bfloat16)


def vmem_call(kernel, out_shape, scalars, arrays, scratch, flops, far=(), sems=0):
    specs = [pl.BlockSpec(memory_space=pltpu.SMEM)] * len(scalars)
    specs += [pl.BlockSpec(memory_space=pltpu.VMEM)] * len(arrays)
    specs += [pl.BlockSpec(memory_space=pltpu.HBM)] * len(far)
    held = [*arrays, *jax.tree.leaves(out_shape), *scratch]
    scratch = scratch + ([pltpu.SemaphoreType.DMA((sems,))] if sems else [])
    grant = sum(math.prod(a.shape) * jnp.dtype(a.dtype).itemsize for a in held) + ROOM
    return pl.pallas_call(
        kernel,
        out_shape=out_shape,
        in_specs=specs,
        out_specs=jax.tree.map(lambda _: pl.BlockSpec(memory_space=pltpu.VMEM), out_shape),
        scratch_shapes=scratch,
        cost_estimate=pl.CostEstimate(flops=flops, bytes_accessed=1 << 20, transcendentals=0),
        compiler_params=pltpu.CompilerParams(vmem_limit_bytes=grant),
    )(*scalars, *arrays, *far)


def fast_body(plan, features, counts, tile_mask, queries, norm_gain, head_scale, w_query, w_kv, w_out):
    layer_count = w_kv.shape[0]
    rows = plan.n_q // plan.n_t
    axes = ("tiles", "heads", "kv")
    devices = [
        (t, h, k) for t in range(plan.n_t) for h in range(plan.n_h) for k in range(plan.n_k)
    ]
    side = lax.axis_index("kv")

    def number(t, h, k):
        return (t * plan.n_h + h) * plan.n_k + k

    def swap(value, axis):
        size = {"heads": plan.n_h, "kv": plan.n_k}[axis]
        return lax.ppermute(value, axis, [(i, i ^ 1) for i in range(size)])

    def exchange(chunks):
        received = []
        for d in range(plan.n_t - 1, 0, -1):
            received.append(lax.ppermute(chunks[d], "tiles", [(i, i ^ d) for i in range(plan.n_t)]))
        shape = jax.ShapeDtypeStruct((rows, plan.width), jnp.bfloat16)
        attended = vmem_call(
            functools.partial(combine_kernel, plan), shape, [], [chunks[0], *received], [], 1 << 20
        )
        partner = swap(attended, "kv")
        low = jnp.where(side == 0, attended, partner)
        high = jnp.where(side == 0, partner, attended)
        lead = plan.start[1]
        overlap = jnp.where(
            lax.broadcasted_iota(jnp.int32, (1, plan.width - lead), 1) < plan.half - lead,
            low[:, lead:],
            high[:, : plan.width - lead],
        )
        return jnp.concatenate([low[:, :lead], overlap, high[:, plan.width - lead :]], axis=1)

    def spread(block):
        received = []
        for pair in plan.rounds:
            links = [
                (number(t, h, k), number(t ^ pair[k][0], h ^ pair[k][1], k))
                for t, h, k in devices
                if pair[k] is not None
            ]
            received.append(lax.ppermute(block, axes, links))
        near = jnp.concatenate(received, axis=0)
        return near, swap(near, "kv")

    def collect(block):
        received = []
        for turn in range(plan.n_h):
            links = []
            for t, h, k in devices:
                source_t, source_h = h * plan.n_k + k, h ^ ((turn + t) % plan.n_h)
                links.append((number(source_t, source_h, (t // plan.n_h) % plan.n_k), number(t, h, k)))
            received.append(lax.ppermute(block, axes, links))
        return received

    weights = w_kv.reshape(layer_count, w_kv.shape[1], plan.cols)
    wq = jnp.swapaxes(w_query, 1, 2)
    q_x = swap(queries, "heads")
    q_k = swap(queries, "kv")
    q_xk = swap(q_x, "kv")
    tied, _ = lax.optimization_barrier((w_out, q_x))
    wo_x = swap(tied, "heads")
    wo = [w_out, swap(w_out, "kv"), wo_x, swap(wo_x, "kv")]
    tiles = features.shape[0]
    bf16, f32 = jnp.bfloat16, jnp.float32
    feat = features.shape[1]
    piece = jax.ShapeDtypeStruct((tiles, plan.width), bf16)
    cost = 2 * tiles * feat * plan.cols
    own, other, near_tiles, later = vmem_call(
        functools.partial(load_project_kernel, plan),
        [
            piece,
            piece,
            jax.ShapeDtypeStruct((tiles, feat), bf16),
            jax.ShapeDtypeStruct((feat, plan.cols), bf16),
        ],
        [counts],
        [tile_mask],
        [pltpu.VMEM((feat, plan.cols), bf16)],
        cost,
        tuple(pltpu.with_memory_space_constraint(a, pltpu.HBM) for a in (features, weights)),
        tile_mask.shape[0] + 2,
    )
    pairs = [(own, swap(other, "kv"))]
    own, other = vmem_call(
        functools.partial(project_kernel, plan),
        [piece, piece],
        [counts],
        [tile_mask, near_tiles, later],
        [],
        cost,
    )
    pairs.append((own, swap(other, "kv")))
    chunk_shapes = [jax.ShapeDtypeStruct((rows, plan.width), f32)]
    chunk_shapes += [jax.ShapeDtypeStruct((rows, plan.width), bf16)] * (plan.n_t - 1)
    wq_scratch = pltpu.VMEM((plan.width, plan.dq), bf16)
    mix_scratch = pltpu.VMEM((plan.n_q, plan.width), f32)
    wo_scratch = pltpu.VMEM((plan.n_h * plan.cols, plan.dq), bf16)

    work = 4 * plan.n_q * tiles * plan.width
    outs = vmem_call(
        functools.partial(first_kernel, plan),
        chunk_shapes + [jax.ShapeDtypeStruct((plan.n_q, plan.dq), bf16)],
        [head_scale],
        [queries, q_k, q_x, q_xk, norm_gain, wq, *pairs[0]],
        [wq_scratch, mix_scratch],
        work,
    )
    chunks, states = outs[: plan.n_t], outs[plan.n_t]
    block = exchange(chunks)
    near, far = spread(block)
    outs = vmem_call(
        functools.partial(layer_kernel, plan, 1),
        chunk_shapes + [jax.ShapeDtypeStruct((plan.q_rows, plan.dq), f32)],
        [head_scale],
        [states, block, near, far, *wo, norm_gain, wq, *pairs[1]],
        [
            pltpu.VMEM((plan.n_h, plan.n_q, plan.cols), bf16),
            wo_scratch,
            pltpu.VMEM((plan.n_q, plan.dq), f32),
            wq_scratch,
            mix_scratch,
        ],
        work,
    )
    chunks, kept = outs[: plan.n_t], outs[plan.n_t]
    block = exchange(chunks)
    near, far = collect(block)
    return vmem_call(
        functools.partial(last_kernel, plan, 1),
        jax.ShapeDtypeStruct((plan.q_rows, plan.dq), f32),
        [],
        [kept, near, far, *wo],
        [pltpu.VMEM((plan.n_h, plan.q_rows, plan.cols), bf16), wo_scratch],
        2 * plan.q_rows * plan.dq * plan.dq,
    )


def solution(mesh):
    def body(features, counts, tile_mask, queries, norm_gain, head_scale, w_query, w_kv, w_out):
        args = (features, counts, tile_mask, queries, norm_gain, head_scale, w_query, w_kv, w_out)
        plan = Plan(mesh, queries, head_scale, w_kv)
        if w_kv.shape[0] == 2 and plan.usable():
            return fast_body(plan, *args)
        return generic_body(*args)

    return jax.shard_map(
        body,
        mesh=mesh,
        in_specs=(
            P(("groups", "tiles"), None),
            P(("groups", "tiles")),
            P(("groups", "tiles"), None),
            P(("heads", "kv"), None),
            P(),
            P("heads"),
            P(None, None, ("heads", "kv")),
            P(None, None, "kv", "heads"),
            P(None, ("heads", "kv"), None),
        ),
        out_specs=P(("groups", "heads", "kv"), None),
        check_vma=False,
    )
```

```python
import functools
import math

import jax
import jax.numpy as jnp
from jax import lax
from jax.experimental import pallas as pl
from jax.experimental.pallas import tpu as pltpu
from jax.sharding import PartitionSpec as P


SOFT_CAP = 50.0
NORM_EPS = 1e-06
LANES = 128
SPLIT = 16
ROOM = 4 << 20


def normalize(hidden, gain_row):
    return (
        hidden * lax.rsqrt(jnp.mean(hidden * hidden, axis=-1, keepdims=True) + NORM_EPS) * gain_row
    )


def generic_body(features, counts, tile_mask, queries, norm_gain, head_scale, w_query, w_kv, w_out):
    slot_count = tile_mask.shape[0]
    block_rows = tile_mask.shape[1]
    total_rows = slot_count * block_rows
    half_rows = total_rows // 2
    layer_count = w_kv.shape[0]
    head_cols = w_kv.shape[3]
    heads_local = head_scale.shape[0]
    head_dim = head_cols // heads_local
    kv_side = lax.axis_index("kv")
    kv_weights = w_kv[:, :, 0, :]
    slot_ids = jnp.arange(slot_count, dtype=jnp.int32)

    def add_block(slot_at, current):
        block_feats = lax.dynamic_slice_in_dim(features, slot_at * block_rows, block_rows, 0)
        result = jnp.einsum(
            "rf,lfc->lrc", block_feats, kv_weights, preferred_element_type=jnp.float32
        )
        return lax.dynamic_update_slice_in_dim(
            current, result.astype(jnp.bfloat16), slot_at * block_rows, 1
        )

    own_count = counts[0]
    projected = jnp.zeros((layer_count, total_rows, head_cols), jnp.bfloat16)
    projected = lax.fori_loop(jnp.int32(0), own_count, add_block, projected)
    live_mask = tile_mask * (slot_ids < own_count).astype(jnp.int32)[:, None]
    kv_local = lax.all_to_all(projected, "kv", split_axis=1, concat_axis=2, tiled=True)
    valid_tiles = lax.dynamic_slice_in_dim(
        live_mask.reshape(total_rows).astype(jnp.float32), kv_side * half_rows, half_rows, 0
    )
    states = queries.astype(jnp.float32)
    scale_vec = head_scale / math.sqrt(head_dim)
    for layer_at in range(layer_count):
        normed = lax.all_gather(
            normalize(states, norm_gain[layer_at]).astype(jnp.bfloat16),
            ("heads", "kv"),
            axis=0,
            tiled=True,
        )
        query_part = jnp.dot(normed, w_query[layer_at], preferred_element_type=jnp.float32).astype(
            jnp.bfloat16
        )
        query_cols = lax.all_gather(query_part, "kv", axis=1, tiled=True)
        n_queries = query_cols.shape[0]
        query_heads = query_cols.reshape(n_queries, heads_local, head_dim)
        key_heads = kv_local[layer_at, :, :head_cols].reshape(half_rows, heads_local, head_dim)
        value_heads = kv_local[layer_at, :, head_cols:].reshape(half_rows, heads_local, head_dim)
        scores = jnp.einsum(
            "qhd,khd->hqk", query_heads, key_heads, preferred_element_type=jnp.float32
        )
        scores = scores * scale_vec[:, None, None]
        capped = SOFT_CAP * jnp.tanh(scores / SOFT_CAP)
        weights_p = jnp.exp(capped) * valid_tiles[None, None, :]
        totals = jnp.sum(weights_p, axis=2)
        partial_value = jnp.einsum(
            "hqk,khd->qhd",
            weights_p.astype(jnp.bfloat16),
            value_heads,
            preferred_element_type=jnp.float32,
        )
        totals, partial_value = lax.psum((totals, partial_value), ("tiles", "kv"))
        attended = (
            (partial_value / jnp.transpose(totals)[:, :, None])
            .reshape(n_queries, head_cols)
            .astype(jnp.bfloat16)
        )
        own_cols = lax.dynamic_slice_in_dim(attended, kv_side * (head_cols // 2), head_cols // 2, 1)
        states = states + lax.psum_scatter(
            jnp.dot(own_cols, w_out[layer_at], preferred_element_type=jnp.float32),
            ("heads", "kv"),
            scatter_dimension=0,
            tiled=True,
        )
    return states


class Plan:
    def __init__(self, mesh, queries, head_scale, w_kv):
        self.n_t, self.n_h, self.n_k = (mesh.shape[a] for a in ("tiles", "heads", "kv"))
        self.q_rows, self.dq = queries.shape
        self.n_q = self.q_rows * self.n_h * self.n_k
        self.cols = w_kv.shape[3]
        self.heads = head_scale.shape[0] // self.n_k
        self.head_dim = self.cols // head_scale.shape[0]
        self.half = self.heads * self.head_dim
        self.width = -(-self.half // LANES) * LANES
        self.start = [k * self.half // LANES * LANES for k in range(self.n_k)]
        self.off = [k * self.half - s for k, s in enumerate(self.start)]
        offsets = [(t, h) for t in range(self.n_t) for h in range(self.n_h)][1:]
        offsets = sorted(offsets, reverse=True)
        offsets += [None] * (-len(offsets) % self.n_k)
        self.rounds = [
            tuple(offsets[i + (k + i // self.n_k) % self.n_k] for k in range(self.n_k))
            for i in range(0, len(offsets), self.n_k)
        ]

    def usable(self):
        return (
            self.n_k == 2
            and self.n_h == 2
            and self.n_t == self.n_h * self.n_k
            and self.half * self.n_k == self.cols
            and self.cols % LANES == 0
            and self.q_rows % 16 == 0
            and self.off[0] == 0
            and all(s + self.width <= self.cols for s in self.start)
            and all(o == 0 or o + self.half == self.width for o in self.off)
            and self.width - self.half >= 2 * SPLIT
            and self.heads <= SPLIT
        )


def place():
    return lax.axis_index("tiles"), lax.axis_index("heads"), lax.axis_index("kv")


def rows_at(index, size):
    return pl.ds(pl.multiple_of(index * size, size), size)


def project_rows(plan, live_ref, feats, weights, own_ref, other_ref, low, high):
    first = lax.axis_index("kv") == 0
    rows = live_ref.shape[1]
    lane = lax.broadcasted_iota(jnp.int32, (1, plan.width), 1)
    acc = jnp.dot(feats[low:high, :], weights[...], preferred_element_type=jnp.float32)
    for slot in range(low // rows, high // rows):
        valid = jnp.broadcast_to(live_ref[slot : slot + 1, :], (LANES, rows)).T
        valid = jnp.concatenate([valid] * (plan.width // LANES), axis=1)
        part = acc[slot * rows - low : slot * rows - low + rows]
        pieces = []
        for start, off in zip(plan.start, plan.off):
            inside = (lane >= off) & (lane < off + plan.half)
            block = part[:, start : start + plan.width]
            pieces.append(jnp.where(inside, block * valid, valid).astype(jnp.bfloat16))
        at = slice(slot * rows, slot * rows + rows)
        own_ref[at, :] = jnp.where(first, pieces[0], pieces[1])
        other_ref[at, :] = jnp.where(first, pieces[1], pieces[0])


def group_of(live_ref):
    slots, rows = live_ref.shape
    return rows * (2 if slots % 2 == 0 else 1)


def load_project_kernel(
    plan,
    count_ref,
    feats_hbm,
    weights_hbm,
    mask_hbm,
    own_ref,
    other_ref,
    feats_ref,
    later_ref,
    live_ref,
    weights_ref,
    mask_ref,
    sems,
):
    size = group_of(live_ref)
    groups = feats_ref.shape[0] // size
    copies = [
        pltpu.make_async_copy(mask_hbm, mask_ref, sems.at[groups + 2]),
        pltpu.make_async_copy(weights_hbm.at[0], weights_ref, sems.at[groups]),
    ]
    for index in range(groups):
        at = pl.ds(index * size, size)
        copies.append(
            pltpu.make_async_copy(feats_hbm.at[at], feats_ref.at[at], sems.at[index])
        )
    copies.append(pltpu.make_async_copy(weights_hbm.at[1], later_ref, sems.at[groups + 1]))
    for copy in copies:
        copy.start()
    copies[0].wait()
    marks = mask_ref[...].astype(jnp.float32)
    slot_ids = lax.broadcasted_iota(jnp.int32, marks.shape, 0)
    live_ref[...] = jnp.where(slot_ids < count_ref[0], marks, 0.0)
    copies[1].wait()
    for index in range(groups):
        copies[2 + index].wait()
        low = index * size
        project_rows(plan, live_ref, feats_ref, weights_ref, own_ref, other_ref, low, low + size)
    copies[-1].wait()


def project_kernel(plan, live_ref, feats_ref, weights_ref, own_ref, other_ref):
    size = group_of(live_ref)
    for low in range(0, feats_ref.shape[0], size):
        project_rows(plan, live_ref, feats_ref, weights_ref, own_ref, other_ref, low, low + size)


def attend(plan, query, scale_ref, own_ref, recv_ref, chunk_refs, mix):
    me_t, _, side = place()
    first = side == 0
    off = jnp.where(first, plan.off[0], plan.off[1])
    pad = jnp.where(first, plan.half if plan.off[0] == 0 else 0, plan.half if plan.off[1] == 0 else 0)
    lane = lax.broadcasted_iota(jnp.int32, (1, plan.width), 1)
    factor = SOFT_CAP * math.log2(math.e)
    n_keys = own_ref.shape[0]
    block = min(n_keys, 512)
    masked, scales = [], []
    for head in range(plan.heads):
        low = off + head * plan.head_dim
        masked.append(
            jnp.where((lane >= low) & (lane < low + plan.head_dim), query, jnp.zeros_like(query))
        )
        scales.append(
            scale_ref[side * plan.heads + head] * (1.0 / (SOFT_CAP * math.sqrt(plan.head_dim)))
        )
    stacked = jnp.concatenate(masked, axis=0)
    for at in range(0, n_keys, block):
        mine = own_ref[at : at + block, :]
        theirs = recv_ref[at : at + block, :]
        keys = jnp.where(first, mine, theirs)
        values = jnp.where(first, theirs, mine)
        scores = lax.dot_general(
            stacked, keys, (((1,), (1,)), ((), ())), preferred_element_type=jnp.float32
        )
        weights = []
        for head, scale in enumerate(scales):
            part = scores[head * plan.n_q : head * plan.n_q + plan.n_q]
            weights.append(jnp.exp2(jnp.tanh(part * scale) * factor).astype(jnp.bfloat16))
        part = jnp.dot(
            jnp.concatenate(weights, axis=0), values, preferred_element_type=jnp.float32
        )
        mix[...] = part if at == 0 else mix[...] + part
    totals = [mix[head * plan.n_q : head * plan.n_q + plan.n_q, :] for head in range(plan.heads)]
    result = jnp.zeros((plan.n_q, plan.width), jnp.float32)
    spot = lane - pad
    spare = (spot >= 0) & (spot < 2 * SPLIT)
    for head in range(plan.heads):
        low = off + head * plan.head_dim
        keep = (lane >= low) & (lane < low + plan.head_dim)
        keep = keep | (spare & (jnp.bitwise_and(spot, SPLIT - 1) == head))
        result = jnp.where(keep, totals[head], result)
    rounded = result.astype(jnp.bfloat16).astype(jnp.float32)
    late = spare & (spot >= SPLIT)
    mix[: plan.n_q, :] = jnp.where(late, result - rounded, rounded)
    for index, ref in enumerate(chunk_refs):
        rows = plan.n_q // plan.n_t
        ref[...] = mix[rows_at(jnp.bitwise_xor(me_t, index), rows), :].astype(ref.dtype)


def query_of(plan, states, gain, wq, wq_pad):
    side = lax.axis_index("kv")
    mean = jnp.mean(states * states, axis=-1, keepdims=True)
    normed = (states * lax.rsqrt(mean + NORM_EPS) * gain).astype(jnp.bfloat16)
    wq_pad[...] = jnp.zeros_like(wq_pad)
    step = max(plan.off)
    wq_pad[pl.ds(pl.multiple_of(side * step, step), plan.half), :] = wq
    return lax.dot_general(
        normed, wq_pad[...], (((1,), (1,)), ((), ())), preferred_element_type=jnp.float32
    ).astype(jnp.bfloat16)


def gather_queries(plan, refs, states_ref):
    _, me_h, me_k = place()
    for dh in range(plan.n_h):
        for dk in range(plan.n_k):
            index = jnp.bitwise_xor(me_h, dh) * plan.n_k + jnp.bitwise_xor(me_k, dk)
            block = refs[dh * plan.n_k + dk][...]
            states_ref[rows_at(index, plan.q_rows), :] = block.astype(jnp.float32)


def first_kernel(
    plan, scale_ref, q_ref, qk_ref, qx_ref, qxk_ref, gain_ref, wq_ref, own_ref, recv_ref, *rest
):
    chunks, (states_ref, wq_pad, mix) = rest[: plan.n_t], rest[plan.n_t :]
    gather_queries(plan, (q_ref, qk_ref, qx_ref, qxk_ref), states_ref)
    query = query_of(plan, states_ref[...], gain_ref[0:1, :], wq_ref[0], wq_pad)
    attend(plan, query, scale_ref, own_ref, recv_ref, chunks, mix)


def fill_out(plan, layer, wo_refs, wo_all):
    me_k = lax.axis_index("kv")
    for dh in range(plan.n_h):
        for dk in range(plan.n_k):
            index = dh * plan.n_k + jnp.bitwise_xor(me_k, dk)
            wo_all[rows_at(index, plan.half), :] = wo_refs[dh * plan.n_k + dk][layer]


def layer_kernel(
    plan,
    layer,
    scale_ref,
    q_ref,
    qk_ref,
    qx_ref,
    qxk_ref,
    block_ref,
    near_ref,
    far_ref,
    wo0,
    wo1,
    wo2,
    wo3,
    gain_ref,
    wq_ref,
    own_hbm,
    recv_hbm,
    *rest,
):
    chunks, rest = rest[: plan.n_t], rest[plan.n_t :]
    kept_ref, att, wo_all, states_ref, wq_pad, mix, own_ref, recv_ref, sems = rest
    copies = [
        pltpu.make_async_copy(own_hbm, own_ref, sems.at[0]),
        pltpu.make_async_copy(recv_hbm, recv_ref, sems.at[1]),
    ]
    for copy in copies:
        copy.start()
    me_t, me_h, me_k = place()
    rows = plan.n_q // plan.n_t
    fill_out(plan, layer - 1, (wo0, wo1, wo2, wo3), wo_all)
    for index, pair in enumerate(plan.rounds):
        for ref, flip in ((near_ref, 0), (far_ref, 1)):
            choice = [pair[k ^ flip] or (0, 0) for k in range(2)]
            dt = jnp.where(me_k == 0, choice[0][0], choice[1][0])
            dh = jnp.where(me_k == 0, choice[0][1], choice[1][1])
            att[rows_at(jnp.bitwise_xor(me_t, dt), rows), rows_at(dh, plan.cols)] = ref[
                index * rows : index * rows + rows, :
            ]
    att[rows_at(me_t, rows), : plan.cols] = block_ref[...]
    out = jnp.dot(att[...], wo_all[...], preferred_element_type=jnp.float32)
    gather_queries(plan, (q_ref, qk_ref, qx_ref, qxk_ref), states_ref)
    states = states_ref[...] + out
    states_ref[...] = states
    kept_ref[...] = states_ref[rows_at(me_h * plan.n_k + me_k, plan.q_rows), :]
    query = query_of(plan, states, gain_ref[layer : layer + 1, :], wq_ref[layer], wq_pad)
    for copy in copies:
        copy.wait()
    attend(plan, query, scale_ref, own_ref, recv_ref, chunks, mix)


def last_kernel(plan, layer, kept_ref, near_ref, far_ref, wo0, wo1, wo2, wo3, out_ref, att, wo_all):
    me_t = lax.axis_index("tiles")
    fill_out(plan, layer, (wo0, wo1, wo2, wo3), wo_all)
    for index, ref in enumerate((near_ref, far_ref)):
        att[:, rows_at((me_t + index) % plan.n_h, plan.cols)] = ref[...]
    out = jnp.dot(att[...], wo_all[...], preferred_element_type=jnp.float32)
    out_ref[...] = kept_ref[...] + out


def combine_kernel(plan, *refs):
    *parts, out_ref = refs
    side = lax.axis_index("kv")
    first = side == 0
    off = jnp.where(first, plan.off[0], plan.off[1])
    pad = jnp.where(first, plan.half if plan.off[0] == 0 else 0, plan.half if plan.off[1] == 0 else 0)
    lane = lax.broadcasted_iota(jnp.int32, (1, plan.width), 1)
    spot = lane - pad
    spare = (spot >= 0) & (spot < 2 * SPLIT)
    total = sum(ref[...].astype(jnp.float32) for ref in parts)
    below = jnp.ones_like(total)
    for head in range(plan.heads):
        low = off + head * plan.head_dim
        mine = spare & (jnp.bitwise_and(spot, SPLIT - 1) == head)
        weight = jnp.sum(jnp.where(mine, total, 0.0), axis=1, keepdims=True)
        below = jnp.where((lane >= low) & (lane < low + plan.head_dim), weight, below)
    out_ref[...] = (total / below).astype(jnp.bfloat16)


def vmem_call(kernel, out_shape, scalars, arrays, scratch, flops, far=(), sems=0):
    specs = [pl.BlockSpec(memory_space=pltpu.SMEM)] * len(scalars)
    specs += [pl.BlockSpec(memory_space=pltpu.VMEM)] * len(arrays)
    specs += [pl.BlockSpec(memory_space=pltpu.HBM)] * len(far)
    held = [*arrays, *jax.tree.leaves(out_shape), *scratch]
    scratch = scratch + ([pltpu.SemaphoreType.DMA((sems,))] if sems else [])
    grant = sum(math.prod(a.shape) * jnp.dtype(a.dtype).itemsize for a in held) + ROOM
    return pl.pallas_call(
        kernel,
        out_shape=out_shape,
        in_specs=specs,
        out_specs=jax.tree.map(lambda _: pl.BlockSpec(memory_space=pltpu.VMEM), out_shape),
        scratch_shapes=scratch,
        cost_estimate=pl.CostEstimate(flops=flops, bytes_accessed=1 << 20, transcendentals=0),
        compiler_params=pltpu.CompilerParams(vmem_limit_bytes=grant),
    )(*scalars, *arrays, *far)


def fast_body(plan, features, counts, tile_mask, queries, norm_gain, head_scale, w_query, w_kv, w_out):
    layer_count = w_kv.shape[0]
    rows = plan.n_q // plan.n_t
    axes = ("tiles", "heads", "kv")
    devices = [
        (t, h, k) for t in range(plan.n_t) for h in range(plan.n_h) for k in range(plan.n_k)
    ]
    side = lax.axis_index("kv")

    def number(t, h, k):
        return (t * plan.n_h + h) * plan.n_k + k

    def swap(value, axis):
        size = {"heads": plan.n_h, "kv": plan.n_k}[axis]
        return lax.ppermute(value, axis, [(i, i ^ 1) for i in range(size)])

    def exchange(chunks):
        received = []
        for d in range(plan.n_t - 1, 0, -1):
            received.append(lax.ppermute(chunks[d], "tiles", [(i, i ^ d) for i in range(plan.n_t)]))
        shape = jax.ShapeDtypeStruct((rows, plan.width), jnp.bfloat16)
        attended = vmem_call(
            functools.partial(combine_kernel, plan), shape, [], [chunks[0], *received], [], 1 << 20
        )
        partner = swap(attended, "kv")
        low = jnp.where(side == 0, attended, partner)
        high = jnp.where(side == 0, partner, attended)
        lead = plan.start[1]
        overlap = jnp.where(
            lax.broadcasted_iota(jnp.int32, (1, plan.width - lead), 1) < plan.half - lead,
            low[:, lead:],
            high[:, : plan.width - lead],
        )
        return jnp.concatenate([low[:, :lead], overlap, high[:, plan.width - lead :]], axis=1)

    def spread(block):
        received = []
        for pair in plan.rounds:
            links = [
                (number(t, h, k), number(t ^ pair[k][0], h ^ pair[k][1], k))
                for t, h, k in devices
                if pair[k] is not None
            ]
            received.append(lax.ppermute(block, axes, links))
        near = jnp.concatenate(received, axis=0)
        return near, swap(near, "kv")

    def collect(block):
        received = []
        for turn in range(plan.n_h):
            links = []
            for t, h, k in devices:
                source_t, source_h = h * plan.n_k + k, h ^ ((turn + t) % plan.n_h)
                links.append((number(source_t, source_h, (t // plan.n_h) % plan.n_k), number(t, h, k)))
            received.append(lax.ppermute(block, axes, links))
        return received

    weights = w_kv.reshape(layer_count, w_kv.shape[1], plan.cols)
    wq = jnp.swapaxes(w_query, 1, 2)
    q_x = swap(queries, "heads")
    q_k = swap(queries, "kv")
    q_xk = swap(q_x, "kv")
    wo_x = swap(w_out, "heads")
    wo = [w_out, swap(w_out, "kv"), wo_x, swap(wo_x, "kv")]
    tiles = features.shape[0]
    bf16, f32 = jnp.bfloat16, jnp.float32
    feat = features.shape[1]
    piece = jax.ShapeDtypeStruct((tiles, plan.width), bf16)
    cost = 2 * tiles * feat * plan.cols
    live_shape = jax.ShapeDtypeStruct(tile_mask.shape, f32)
    own, other, near_tiles, later, live = vmem_call(
        functools.partial(load_project_kernel, plan),
        [
            piece,
            piece,
            jax.ShapeDtypeStruct((tiles, feat), bf16),
            jax.ShapeDtypeStruct((feat, plan.cols), bf16),
            live_shape,
        ],
        [counts],
        [],
        [
            pltpu.VMEM((feat, plan.cols), bf16),
            pltpu.VMEM(tile_mask.shape, jnp.int32),
        ],
        cost,
        [
            pltpu.with_memory_space_constraint(a, pltpu.HBM)
            for a in (features, weights, tile_mask)
        ],
        tile_mask.shape[0] + 3,
    )
    pairs = [(own, swap(other, "kv"))]
    own, other = vmem_call(
        functools.partial(project_kernel, plan),
        [piece, piece],
        [],
        [live, near_tiles, later],
        [],
        cost,
    )
    pairs.append((own, swap(other, "kv")))

    chunk_shapes = [jax.ShapeDtypeStruct((rows, plan.width), f32)]
    chunk_shapes += [jax.ShapeDtypeStruct((rows, plan.width), bf16)] * (plan.n_t - 1)
    wq_scratch = pltpu.VMEM((plan.width, plan.dq), bf16)
    states_scratch = pltpu.VMEM((plan.n_q, plan.dq), f32)
    mix_scratch = pltpu.VMEM((plan.heads * plan.n_q, plan.width), f32)
    wo_scratch = pltpu.VMEM((plan.n_h * plan.cols, plan.dq), bf16)

    work = 4 * plan.n_q * tiles * plan.width
    chunks = vmem_call(
        functools.partial(first_kernel, plan),
        chunk_shapes,
        [head_scale],
        [queries, q_k, q_x, q_xk, norm_gain, wq, *pairs[0]],
        [states_scratch, wq_scratch, mix_scratch],
        work,
    )
    block = exchange(chunks)
    near, far = spread(block)
    outs = vmem_call(
        functools.partial(layer_kernel, plan, 1),
        chunk_shapes + [jax.ShapeDtypeStruct((plan.q_rows, plan.dq), f32)],
        [head_scale],
        [queries, q_k, q_x, q_xk, block, near, far, *wo, norm_gain, wq],
        [
            pltpu.VMEM((plan.n_q, plan.n_h * plan.cols), bf16),
            wo_scratch,
            states_scratch,
            wq_scratch,
            mix_scratch,
            pltpu.VMEM((tiles, plan.width), bf16),
            pltpu.VMEM((tiles, plan.width), bf16),
        ],
        work,
        [pltpu.with_memory_space_constraint(a, pltpu.HBM) for a in pairs[1]],
        2,
    )
    chunks, kept = outs[: plan.n_t], outs[plan.n_t]
    block = exchange(chunks)
    near, far = collect(block)
    return vmem_call(
        functools.partial(last_kernel, plan, 1),
        jax.ShapeDtypeStruct((plan.q_rows, plan.dq), f32),
        [],
        [kept, near, far, *wo],
        [pltpu.VMEM((plan.q_rows, plan.n_h * plan.cols), bf16), wo_scratch],
        2 * plan.q_rows * plan.dq * plan.dq,
    )


def solution(mesh):
    def body(features, counts, tile_mask, queries, norm_gain, head_scale, w_query, w_kv, w_out):
        args = (features, counts, tile_mask, queries, norm_gain, head_scale, w_query, w_kv, w_out)
        plan = Plan(mesh, queries, head_scale, w_kv)
        if w_kv.shape[0] == 2 and plan.usable():
            return fast_body(plan, *args)
        return generic_body(*args)

    return jax.shard_map(
        body,
        mesh=mesh,
        in_specs=(
            P(("groups", "tiles"), None),
            P(("groups", "tiles")),
            P(("groups", "tiles"), None),
            P(("heads", "kv"), None),
            P(),
            P("heads"),
            P(None, None, ("heads", "kv")),
            P(None, None, "kv", "heads"),
            P(None, ("heads", "kv"), None),
        ),
        out_specs=P(("groups", "heads", "kv"), None),
        check_vma=False,
    )
```

```python
import functools
import math

import jax
import jax.numpy as jnp
from jax import lax
from jax.experimental import pallas as pl
from jax.experimental.pallas import tpu as pltpu
from jax.sharding import PartitionSpec as P


SOFT_CAP = 50.0
NORM_EPS = 1e-06
LANES = 128
SPLIT = 16
ROOM = 4 << 20


def normalize(hidden, gain_row):
    return (
        hidden * lax.rsqrt(jnp.mean(hidden * hidden, axis=-1, keepdims=True) + NORM_EPS) * gain_row
    )


def generic_body(features, counts, tile_mask, queries, norm_gain, head_scale, w_query, w_kv, w_out):
    slot_count = tile_mask.shape[0]
    block_rows = tile_mask.shape[1]
    total_rows = slot_count * block_rows
    half_rows = total_rows // 2
    layer_count = w_kv.shape[0]
    head_cols = w_kv.shape[3]
    heads_local = head_scale.shape[0]
    head_dim = head_cols // heads_local
    kv_side = lax.axis_index("kv")
    kv_weights = w_kv[:, :, 0, :]
    slot_ids = jnp.arange(slot_count, dtype=jnp.int32)

    def add_block(slot_at, current):
        block_feats = lax.dynamic_slice_in_dim(features, slot_at * block_rows, block_rows, 0)
        result = jnp.einsum(
            "rf,lfc->lrc", block_feats, kv_weights, preferred_element_type=jnp.float32
        )
        return lax.dynamic_update_slice_in_dim(
            current, result.astype(jnp.bfloat16), slot_at * block_rows, 1
        )

    own_count = counts[0]
    projected = jnp.zeros((layer_count, total_rows, head_cols), jnp.bfloat16)
    projected = lax.fori_loop(jnp.int32(0), own_count, add_block, projected)
    live_mask = tile_mask * (slot_ids < own_count).astype(jnp.int32)[:, None]
    kv_local = lax.all_to_all(projected, "kv", split_axis=1, concat_axis=2, tiled=True)
    valid_tiles = lax.dynamic_slice_in_dim(
        live_mask.reshape(total_rows).astype(jnp.float32), kv_side * half_rows, half_rows, 0
    )
    states = queries.astype(jnp.float32)
    scale_vec = head_scale / math.sqrt(head_dim)
    for layer_at in range(layer_count):
        normed = lax.all_gather(
            normalize(states, norm_gain[layer_at]).astype(jnp.bfloat16),
            ("heads", "kv"),
            axis=0,
            tiled=True,
        )
        query_part = jnp.dot(normed, w_query[layer_at], preferred_element_type=jnp.float32).astype(
            jnp.bfloat16
        )
        query_cols = lax.all_gather(query_part, "kv", axis=1, tiled=True)
        n_queries = query_cols.shape[0]
        query_heads = query_cols.reshape(n_queries, heads_local, head_dim)
        key_heads = kv_local[layer_at, :, :head_cols].reshape(half_rows, heads_local, head_dim)
        value_heads = kv_local[layer_at, :, head_cols:].reshape(half_rows, heads_local, head_dim)
        scores = jnp.einsum(
            "qhd,khd->hqk", query_heads, key_heads, preferred_element_type=jnp.float32
        )
        scores = scores * scale_vec[:, None, None]
        capped = SOFT_CAP * jnp.tanh(scores / SOFT_CAP)
        weights_p = jnp.exp(capped) * valid_tiles[None, None, :]
        totals = jnp.sum(weights_p, axis=2)
        partial_value = jnp.einsum(
            "hqk,khd->qhd",
            weights_p.astype(jnp.bfloat16),
            value_heads,
            preferred_element_type=jnp.float32,
        )
        totals, partial_value = lax.psum((totals, partial_value), ("tiles", "kv"))
        attended = (
            (partial_value / jnp.transpose(totals)[:, :, None])
            .reshape(n_queries, head_cols)
            .astype(jnp.bfloat16)
        )
        own_cols = lax.dynamic_slice_in_dim(attended, kv_side * (head_cols // 2), head_cols // 2, 1)
        states = states + lax.psum_scatter(
            jnp.dot(own_cols, w_out[layer_at], preferred_element_type=jnp.float32),
            ("heads", "kv"),
            scatter_dimension=0,
            tiled=True,
        )
    return states


class Plan:
    def __init__(self, mesh, queries, head_scale, w_kv):
        self.n_t, self.n_h, self.n_k = (mesh.shape[a] for a in ("tiles", "heads", "kv"))
        self.q_rows, self.dq = queries.shape
        self.n_q = self.q_rows * self.n_h * self.n_k
        self.cols = w_kv.shape[3]
        self.heads = head_scale.shape[0] // self.n_k
        self.head_dim = self.cols // head_scale.shape[0]
        self.half = self.heads * self.head_dim
        self.width = -(-self.half // LANES) * LANES
        self.start = [k * self.half // LANES * LANES for k in range(self.n_k)]
        self.off = [k * self.half - s for k, s in enumerate(self.start)]
        offsets = [(t, h) for t in range(self.n_t) for h in range(self.n_h)][1:]
        offsets = sorted(offsets, reverse=True)
        offsets += [None] * (-len(offsets) % self.n_k)
        self.rounds = [
            tuple(offsets[i + (k + i // self.n_k) % self.n_k] for k in range(self.n_k))
            for i in range(0, len(offsets), self.n_k)
        ]
        self.rounds = self.rounds[-1:] + self.rounds[:-1]

    def usable(self):
        return (
            self.n_k == 2
            and self.n_h == 2
            and self.n_t == self.n_h * self.n_k
            and self.half * self.n_k == self.cols
            and self.cols % LANES == 0
            and self.q_rows % 16 == 0
            and self.off[0] == 0
            and all(s + self.width <= self.cols for s in self.start)
            and all(o == 0 or o + self.half == self.width for o in self.off)
            and self.width - self.half >= 2 * SPLIT
            and self.heads <= SPLIT
        )


def place():
    return lax.axis_index("tiles"), lax.axis_index("heads"), lax.axis_index("kv")


def rows_at(index, size):
    return pl.ds(pl.multiple_of(index * size, size), size)


def project_rows(plan, live_ref, feats, weights, own_ref, other_ref, low, high):
    first = lax.axis_index("kv") == 0
    rows = live_ref.shape[1]
    lane = lax.broadcasted_iota(jnp.int32, (1, plan.width), 1)
    acc = jnp.dot(feats[low:high, :], weights[...], preferred_element_type=jnp.float32)
    for slot in range(low // rows, high // rows):
        valid = jnp.broadcast_to(live_ref[slot : slot + 1, :], (LANES, rows)).T
        valid = jnp.concatenate([valid] * (plan.width // LANES), axis=1)
        part = acc[slot * rows - low : slot * rows - low + rows]
        pieces = []
        for start, off in zip(plan.start, plan.off):
            inside = (lane >= off) & (lane < off + plan.half)
            block = part[:, start : start + plan.width]
            pieces.append(jnp.where(inside, block * valid, valid).astype(jnp.bfloat16))
        at = slice(slot * rows, slot * rows + rows)
        own_ref[at, :] = jnp.where(first, pieces[0], pieces[1])
        other_ref[at, :] = jnp.where(first, pieces[1], pieces[0])


def group_of(live_ref):
    slots, rows = live_ref.shape
    return rows * (2 if slots % 2 == 0 else 1)


def project_kernel(
    plan,
    layer,
    count_ref,
    feats_hbm,
    weights_hbm,
    mask_hbm,
    own_ref,
    other_ref,
    feats_ref,
    weights_ref,
    mask_ref,
    live_ref,
    sems,
):
    size = group_of(live_ref)
    groups = feats_ref.shape[0] // size
    copies = [
        pltpu.make_async_copy(mask_hbm, mask_ref, sems.at[groups + 1]),
        pltpu.make_async_copy(weights_hbm.at[layer], weights_ref, sems.at[groups]),
    ]
    for index in range(groups):
        at = pl.ds(index * size, size)
        copies.append(
            pltpu.make_async_copy(feats_hbm.at[at], feats_ref.at[at], sems.at[index])
        )
    for copy in copies:
        copy.start()
    copies[0].wait()
    marks = mask_ref[...].astype(jnp.float32)
    slot_ids = lax.broadcasted_iota(jnp.int32, marks.shape, 0)
    live_ref[...] = jnp.where(slot_ids < count_ref[0], marks, 0.0)
    copies[1].wait()
    for index in range(groups):
        copies[2 + index].wait()
        low = index * size
        project_rows(plan, live_ref, feats_ref, weights_ref, own_ref, other_ref, low, low + size)


def attend(plan, query, scale_ref, own_ref, recv_ref, chunk_refs, mix):
    me_t, _, side = place()
    first = side == 0
    off = jnp.where(first, plan.off[0], plan.off[1])
    pad = jnp.where(first, plan.half if plan.off[0] == 0 else 0, plan.half if plan.off[1] == 0 else 0)
    lane = lax.broadcasted_iota(jnp.int32, (1, plan.width), 1)
    factor = SOFT_CAP * math.log2(math.e)
    n_keys = own_ref.shape[0]
    block = min(n_keys, 512)
    masked, scales = [], []
    for head in range(plan.heads):
        low = off + head * plan.head_dim
        masked.append(
            jnp.where((lane >= low) & (lane < low + plan.head_dim), query, jnp.zeros_like(query))
        )
        scales.append(
            scale_ref[side * plan.heads + head] * (1.0 / (SOFT_CAP * math.sqrt(plan.head_dim)))
        )
    stacked = jnp.concatenate(masked, axis=0)
    for at in range(0, n_keys, block):
        mine = own_ref[at : at + block, :]
        theirs = recv_ref[at : at + block, :]
        keys = jnp.where(first, mine, theirs)
        values = jnp.where(first, theirs, mine)
        scores = lax.dot_general(
            stacked, keys, (((1,), (1,)), ((), ())), preferred_element_type=jnp.float32
        )
        weights = []
        for head, scale in enumerate(scales):
            part = scores[head * plan.n_q : head * plan.n_q + plan.n_q]
            weights.append(jnp.exp2(jnp.tanh(part * scale) * factor).astype(jnp.bfloat16))
        part = jnp.dot(
            jnp.concatenate(weights, axis=0), values, preferred_element_type=jnp.float32
        )
        mix[...] = part if at == 0 else mix[...] + part
    totals = [mix[head * plan.n_q : head * plan.n_q + plan.n_q, :] for head in range(plan.heads)]
    result = jnp.zeros((plan.n_q, plan.width), jnp.float32)
    spot = lane - pad
    spare = (spot >= 0) & (spot < 2 * SPLIT)
    for head in range(plan.heads):
        low = off + head * plan.head_dim
        keep = (lane >= low) & (lane < low + plan.head_dim)
        keep = keep | (spare & (jnp.bitwise_and(spot, SPLIT - 1) == head))
        result = jnp.where(keep, totals[head], result)
    rounded = result.astype(jnp.bfloat16).astype(jnp.float32)
    late = spare & (spot >= SPLIT)
    mix[: plan.n_q, :] = jnp.where(late, result - rounded, rounded)
    for index, ref in enumerate(chunk_refs):
        rows = plan.n_q // plan.n_t
        ref[...] = mix[rows_at(jnp.bitwise_xor(me_t, index), rows), :].astype(ref.dtype)


def query_of(plan, states, gain, wq, wq_pad):
    side = lax.axis_index("kv")
    mean = jnp.mean(states * states, axis=-1, keepdims=True)
    normed = (states * lax.rsqrt(mean + NORM_EPS) * gain).astype(jnp.bfloat16)
    wq_pad[...] = jnp.zeros_like(wq_pad)
    step = max(plan.off)
    wq_pad[pl.ds(pl.multiple_of(side * step, step), plan.half), :] = wq
    return lax.dot_general(
        normed, wq_pad[...], (((1,), (1,)), ((), ())), preferred_element_type=jnp.float32
    ).astype(jnp.bfloat16)


def gather_queries(plan, refs, states_ref):
    _, me_h, me_k = place()
    for dh in range(plan.n_h):
        for dk in range(plan.n_k):
            index = jnp.bitwise_xor(me_h, dh) * plan.n_k + jnp.bitwise_xor(me_k, dk)
            block = refs[dh * plan.n_k + dk][...]
            states_ref[rows_at(index, plan.q_rows), :] = block.astype(jnp.float32)


def first_kernel(
    plan, scale_ref, q_ref, qk_ref, qx_ref, qxk_ref, gain_ref, wq_ref, own_ref, recv_ref, *rest
):
    chunks, (states_ref, wq_pad, mix) = rest[: plan.n_t], rest[plan.n_t :]
    gather_queries(plan, (q_ref, qk_ref, qx_ref, qxk_ref), states_ref)
    query = query_of(plan, states_ref[...], gain_ref[0:1, :], wq_ref[0], wq_pad)
    attend(plan, query, scale_ref, own_ref, recv_ref, chunks, mix)


def fill_out(plan, layer, wo_refs, wo_all):
    me_k = lax.axis_index("kv")
    for dh in range(plan.n_h):
        for dk in range(plan.n_k):
            index = dh * plan.n_k + jnp.bitwise_xor(me_k, dk)
            wo_all[rows_at(index, plan.half), :] = wo_refs[dh * plan.n_k + dk][layer]


def layer_kernel(
    plan,
    layer,
    scale_ref,
    q_ref,
    qk_ref,
    qx_ref,
    qxk_ref,
    block_ref,
    near_ref,
    far_ref,
    wo0,
    wo1,
    wo2,
    wo3,
    gain_ref,
    wq_ref,
    own_ref,
    recv_ref,
    *rest,
):
    chunks, rest = rest[: plan.n_t], rest[plan.n_t :]
    kept_ref, att, wo_all, states_ref, wq_pad, mix = rest
    me_t, me_h, me_k = place()
    rows = plan.n_q // plan.n_t
    fill_out(plan, layer - 1, (wo0, wo1, wo2, wo3), wo_all)
    for index, pair in enumerate(plan.rounds):
        for ref, flip in ((near_ref, 0), (far_ref, 1)):
            choice = [pair[k ^ flip] or (0, 0) for k in range(2)]
            dt = jnp.where(me_k == 0, choice[0][0], choice[1][0])
            dh = jnp.where(me_k == 0, choice[0][1], choice[1][1])
            att[rows_at(jnp.bitwise_xor(me_t, dt), rows), rows_at(dh, plan.cols)] = ref[
                index * rows : index * rows + rows, :
            ]
    att[rows_at(me_t, rows), : plan.cols] = block_ref[...]
    out = jnp.dot(att[...], wo_all[...], preferred_element_type=jnp.float32)
    gather_queries(plan, (q_ref, qk_ref, qx_ref, qxk_ref), states_ref)
    states = states_ref[...] + out
    states_ref[...] = states
    kept_ref[...] = states_ref[rows_at(me_h * plan.n_k + me_k, plan.q_rows), :]
    query = query_of(plan, states, gain_ref[layer : layer + 1, :], wq_ref[layer], wq_pad)
    attend(plan, query, scale_ref, own_ref, recv_ref, chunks, mix)


def last_kernel(plan, layer, kept_ref, near_ref, far_ref, wo0, wo1, wo2, wo3, out_ref, att, wo_all):
    me_t = lax.axis_index("tiles")
    fill_out(plan, layer, (wo0, wo1, wo2, wo3), wo_all)
    for index, ref in enumerate((near_ref, far_ref)):
        att[:, rows_at((me_t // plan.n_k + index) % plan.n_h, plan.cols)] = ref[...]
    out = jnp.dot(att[...], wo_all[...], preferred_element_type=jnp.float32)
    out_ref[...] = kept_ref[...] + out


def combine_kernel(plan, *refs):
    *parts, out_ref = refs
    side = lax.axis_index("kv")
    first = side == 0
    off = jnp.where(first, plan.off[0], plan.off[1])
    pad = jnp.where(first, plan.half if plan.off[0] == 0 else 0, plan.half if plan.off[1] == 0 else 0)
    lane = lax.broadcasted_iota(jnp.int32, (1, plan.width), 1)
    spot = lane - pad
    spare = (spot >= 0) & (spot < 2 * SPLIT)
    total = sum(ref[...].astype(jnp.float32) for ref in parts)
    below = jnp.ones_like(total)
    for head in range(plan.heads):
        low = off + head * plan.head_dim
        mine = spare & (jnp.bitwise_and(spot, SPLIT - 1) == head)
        weight = jnp.sum(jnp.where(mine, total, 0.0), axis=1, keepdims=True)
        below = jnp.where((lane >= low) & (lane < low + plan.head_dim), weight, below)
    out_ref[...] = (total / below).astype(jnp.bfloat16)


def vmem_call(kernel, out_shape, scalars, arrays, scratch, flops, far=(), sems=0):
    specs = [pl.BlockSpec(memory_space=pltpu.SMEM)] * len(scalars)
    specs += [pl.BlockSpec(memory_space=pltpu.VMEM)] * len(arrays)
    specs += [pl.BlockSpec(memory_space=pltpu.HBM)] * len(far)
    held = [*arrays, *jax.tree.leaves(out_shape), *scratch]
    scratch = scratch + ([pltpu.SemaphoreType.DMA((sems,))] if sems else [])
    grant = sum(math.prod(a.shape) * jnp.dtype(a.dtype).itemsize for a in held) + ROOM
    return pl.pallas_call(
        kernel,
        out_shape=out_shape,
        in_specs=specs,
        out_specs=[pl.BlockSpec(memory_space=pltpu.VMEM) for _ in out_shape]
        if isinstance(out_shape, list)
        else pl.BlockSpec(memory_space=pltpu.VMEM),
        scratch_shapes=scratch,
        cost_estimate=pl.CostEstimate(flops=flops, bytes_accessed=1 << 20, transcendentals=0),
        compiler_params=pltpu.CompilerParams(vmem_limit_bytes=grant),
    )(*scalars, *arrays, *far)


def fast_body(plan, features, counts, tile_mask, queries, norm_gain, head_scale, w_query, w_kv, w_out):
    layer_count = w_kv.shape[0]
    rows = plan.n_q // plan.n_t
    axes = ("tiles", "heads", "kv")
    devices = [
        (t, h, k) for t in range(plan.n_t) for h in range(plan.n_h) for k in range(plan.n_k)
    ]
    side = lax.axis_index("kv")

    def number(t, h, k):
        return (t * plan.n_h + h) * plan.n_k + k

    def swap(value, axis):
        size = {"heads": plan.n_h, "kv": plan.n_k}[axis]
        return lax.ppermute(value, axis, [(i, i ^ 1) for i in range(size)])

    def exchange(chunks):
        received = []
        for d in range(plan.n_t - 1, 0, -1):
            received.append(lax.ppermute(chunks[d], "tiles", [(i, i ^ d) for i in range(plan.n_t)]))
        shape = jax.ShapeDtypeStruct((rows, plan.width), jnp.bfloat16)
        attended = vmem_call(
            functools.partial(combine_kernel, plan), shape, [], [chunks[0], *received], [], 1 << 20
        )
        partner = swap(attended, "kv")
        low = jnp.where(side == 0, attended, partner)
        high = jnp.where(side == 0, partner, attended)
        lead = plan.start[1]
        overlap = jnp.where(
            lax.broadcasted_iota(jnp.int32, (1, plan.width - lead), 1) < plan.half - lead,
            low[:, lead:],
            high[:, : plan.width - lead],
        )
        return jnp.concatenate([low[:, :lead], overlap, high[:, plan.width - lead :]], axis=1)

    def spread(block):
        received = []
        for pair in plan.rounds:
            links = [
                (number(t, h, k), number(t ^ pair[k][0], h ^ pair[k][1], k))
                for t, h, k in devices
                if pair[k] is not None
            ]
            received.append(lax.ppermute(block, axes, links))
        near = jnp.concatenate(received, axis=0)
        return near, swap(near, "kv")

    def collect(block):
        received = []
        for turn in range(plan.n_h):
            links = []
            for t, h, k in devices:
                source_t = h * plan.n_k + k
                source_h = h ^ ((turn + t // plan.n_k) % plan.n_h)
                source_k = plan.n_k - 1 - t % plan.n_k
                links.append((number(source_t, source_h, source_k), number(t, h, k)))
            received.append(lax.ppermute(block, axes, links))
        return received

    weights = w_kv.reshape(layer_count, w_kv.shape[1], plan.cols)
    wq = jnp.swapaxes(w_query, 1, 2)
    q_x = swap(queries, "heads")
    q_k = swap(queries, "kv")
    q_xk = swap(q_x, "kv")
    wo_x = swap(w_out, "heads")
    wo = [w_out, swap(w_out, "kv"), wo_x, swap(wo_x, "kv")]
    tiles = features.shape[0]
    bf16, f32 = jnp.bfloat16, jnp.float32
    feat = features.shape[1]
    piece = jax.ShapeDtypeStruct((tiles, plan.width), bf16)
    cost = 2 * tiles * feat * plan.cols
    streamed = [
        pltpu.with_memory_space_constraint(a, pltpu.HBM) for a in (features, weights, tile_mask)
    ]
    pairs = []
    for layer in range(layer_count):
        own, other = vmem_call(
            functools.partial(project_kernel, plan, layer),
            [piece, piece],
            [counts],
            [],
            [
                pltpu.VMEM((tiles, feat), bf16),
                pltpu.VMEM((feat, plan.cols), bf16),
                pltpu.VMEM(tile_mask.shape, jnp.int32),
                pltpu.VMEM(tile_mask.shape, f32),
            ],
            cost,
            streamed,
            tile_mask.shape[0] + 2,
        )
        pairs.append((own, swap(other, "kv")))

    chunk_shapes = [jax.ShapeDtypeStruct((rows, plan.width), f32)]
    chunk_shapes += [jax.ShapeDtypeStruct((rows, plan.width), bf16)] * (plan.n_t - 1)
    wq_scratch = pltpu.VMEM((plan.width, plan.dq), bf16)
    states_scratch = pltpu.VMEM((plan.n_q, plan.dq), f32)
    mix_scratch = pltpu.VMEM((plan.heads * plan.n_q, plan.width), f32)
    wo_scratch = pltpu.VMEM((plan.n_h * plan.cols, plan.dq), bf16)

    work = 4 * plan.n_q * tiles * plan.width
    chunks = vmem_call(
        functools.partial(first_kernel, plan),
        chunk_shapes,
        [head_scale],
        [queries, q_k, q_x, q_xk, norm_gain, wq, *pairs[0]],
        [states_scratch, wq_scratch, mix_scratch],
        work,
    )
    block = exchange(chunks)
    near, far = spread(block)
    outs = vmem_call(
        functools.partial(layer_kernel, plan, 1),
        chunk_shapes + [jax.ShapeDtypeStruct((plan.q_rows, plan.dq), f32)],
        [head_scale],
        [queries, q_k, q_x, q_xk, block, near, far, *wo, norm_gain, wq]
        + [pltpu.with_memory_space_constraint(a, pltpu.VMEM) for a in pairs[1]],
        [
            pltpu.VMEM((plan.n_q, plan.n_h * plan.cols), bf16),
            wo_scratch,
            states_scratch,
            wq_scratch,
            mix_scratch,
        ],
        work,
    )
    chunks, kept = outs[: plan.n_t], outs[plan.n_t]
    block = exchange(chunks)
    near, far = collect(block)
    return vmem_call(
        functools.partial(last_kernel, plan, 1),
        jax.ShapeDtypeStruct((plan.q_rows, plan.dq), f32),
        [],
        [kept, near, far, *wo],
        [pltpu.VMEM((plan.q_rows, plan.n_h * plan.cols), bf16), wo_scratch],
        2 * plan.q_rows * plan.dq * plan.dq,
    )


def solution(mesh):
    def body(features, counts, tile_mask, queries, norm_gain, head_scale, w_query, w_kv, w_out):
        args = (features, counts, tile_mask, queries, norm_gain, head_scale, w_query, w_kv, w_out)
        plan = Plan(mesh, queries, head_scale, w_kv)
        if w_kv.shape[0] == 2 and plan.usable():
            return fast_body(plan, *args)
        return generic_body(*args)

    return jax.shard_map(
        body,
        mesh=mesh,
        in_specs=(
            P(("groups", "tiles"), None),
            P(("groups", "tiles")),
            P(("groups", "tiles"), None),
            P(("heads", "kv"), None),
            P(),
            P("heads"),
            P(None, None, ("heads", "kv")),
            P(None, None, "kv", "heads"),
            P(None, ("heads", "kv"), None),
        ),
        out_specs=P(("groups", "heads", "kv"), None),
        check_vma=False,
    )
```

```python
import functools
import math

import jax
import jax.numpy as jnp
from jax import lax
from jax.experimental import pallas as pl
from jax.experimental.pallas import tpu as pltpu
from jax.sharding import PartitionSpec as P


SOFT_CAP = 50.0
NORM_EPS = 1e-06
LANES = 128
SPLIT = 16
ROOM = 4 << 20


def normalize(hidden, gain_row):
    return (
        hidden * lax.rsqrt(jnp.mean(hidden * hidden, axis=-1, keepdims=True) + NORM_EPS) * gain_row
    )


def generic_body(features, counts, tile_mask, queries, norm_gain, head_scale, w_query, w_kv, w_out):
    slot_count = tile_mask.shape[0]
    block_rows = tile_mask.shape[1]
    total_rows = slot_count * block_rows
    half_rows = total_rows // 2
    layer_count = w_kv.shape[0]
    head_cols = w_kv.shape[3]
    heads_local = head_scale.shape[0]
    head_dim = head_cols // heads_local
    kv_side = lax.axis_index("kv")
    kv_weights = w_kv[:, :, 0, :]
    slot_ids = jnp.arange(slot_count, dtype=jnp.int32)

    def add_block(slot_at, current):
        block_feats = lax.dynamic_slice_in_dim(features, slot_at * block_rows, block_rows, 0)
        result = jnp.einsum(
            "rf,lfc->lrc", block_feats, kv_weights, preferred_element_type=jnp.float32
        )
        return lax.dynamic_update_slice_in_dim(
            current, result.astype(jnp.bfloat16), slot_at * block_rows, 1
        )

    own_count = counts[0]
    projected = jnp.zeros((layer_count, total_rows, head_cols), jnp.bfloat16)
    projected = lax.fori_loop(jnp.int32(0), own_count, add_block, projected)
    live_mask = tile_mask * (slot_ids < own_count).astype(jnp.int32)[:, None]
    kv_local = lax.all_to_all(projected, "kv", split_axis=1, concat_axis=2, tiled=True)
    valid_tiles = lax.dynamic_slice_in_dim(
        live_mask.reshape(total_rows).astype(jnp.float32), kv_side * half_rows, half_rows, 0
    )
    states = queries.astype(jnp.float32)
    scale_vec = head_scale / math.sqrt(head_dim)
    for layer_at in range(layer_count):
        normed = lax.all_gather(
            normalize(states, norm_gain[layer_at]).astype(jnp.bfloat16),
            ("heads", "kv"),
            axis=0,
            tiled=True,
        )
        query_part = jnp.dot(normed, w_query[layer_at], preferred_element_type=jnp.float32).astype(
            jnp.bfloat16
        )
        query_cols = lax.all_gather(query_part, "kv", axis=1, tiled=True)
        n_queries = query_cols.shape[0]
        query_heads = query_cols.reshape(n_queries, heads_local, head_dim)
        key_heads = kv_local[layer_at, :, :head_cols].reshape(half_rows, heads_local, head_dim)
        value_heads = kv_local[layer_at, :, head_cols:].reshape(half_rows, heads_local, head_dim)
        scores = jnp.einsum(
            "qhd,khd->hqk", query_heads, key_heads, preferred_element_type=jnp.float32
        )
        scores = scores * scale_vec[:, None, None]
        capped = SOFT_CAP * jnp.tanh(scores / SOFT_CAP)
        weights_p = jnp.exp(capped) * valid_tiles[None, None, :]
        totals = jnp.sum(weights_p, axis=2)
        partial_value = jnp.einsum(
            "hqk,khd->qhd",
            weights_p.astype(jnp.bfloat16),
            value_heads,
            preferred_element_type=jnp.float32,
        )
        totals, partial_value = lax.psum((totals, partial_value), ("tiles", "kv"))
        attended = (
            (partial_value / jnp.transpose(totals)[:, :, None])
            .reshape(n_queries, head_cols)
            .astype(jnp.bfloat16)
        )
        own_cols = lax.dynamic_slice_in_dim(attended, kv_side * (head_cols // 2), head_cols // 2, 1)
        states = states + lax.psum_scatter(
            jnp.dot(own_cols, w_out[layer_at], preferred_element_type=jnp.float32),
            ("heads", "kv"),
            scatter_dimension=0,
            tiled=True,
        )
    return states


class Plan:
    def __init__(self, mesh, queries, head_scale, w_kv):
        self.n_t, self.n_h, self.n_k = (mesh.shape[a] for a in ("tiles", "heads", "kv"))
        self.q_rows, self.dq = queries.shape
        self.n_q = self.q_rows * self.n_h * self.n_k
        self.cols = w_kv.shape[3]
        self.heads = head_scale.shape[0] // self.n_k
        self.head_dim = self.cols // head_scale.shape[0]
        self.half = self.heads * self.head_dim
        self.width = -(-self.half // LANES) * LANES
        self.start = [k * self.half // LANES * LANES for k in range(self.n_k)]
        self.off = [k * self.half - s for k, s in enumerate(self.start)]
        steps = [1, *range(self.n_t - 1, 1, -1)]
        self.rounds = [
            tuple((step, (k + index) % 2) for k in range(self.n_k))
            for index, step in enumerate(steps)
        ]
        self.rounds.append((None,) * (self.n_k - 1) + ((0, 1),))

    def usable(self):
        return (
            self.n_k == 2
            and self.n_h == 2
            and self.n_t == self.n_h * self.n_k
            and self.half * self.n_k == self.cols
            and self.cols % LANES == 0
            and self.q_rows % 16 == 0
            and self.off[0] == 0
            and all(s + self.width <= self.cols for s in self.start)
            and all(o == 0 or o + self.half == self.width for o in self.off)
            and self.width - self.half >= 2 * SPLIT
            and self.heads <= SPLIT
        )


def place():
    return lax.axis_index("tiles"), lax.axis_index("heads"), lax.axis_index("kv")


def rows_at(index, size):
    return pl.ds(pl.multiple_of(index * size, size), size)


def project_rows(plan, live_ref, feats, weights, own_ref, other_ref, low, high):
    first = lax.axis_index("kv") == 0
    rows = live_ref.shape[1]
    lane = lax.broadcasted_iota(jnp.int32, (1, plan.width), 1)
    acc = jnp.dot(feats[low:high, :], weights[...], preferred_element_type=jnp.float32)
    for slot in range(low // rows, high // rows):
        valid = jnp.broadcast_to(live_ref[slot : slot + 1, :], (LANES, rows)).T
        valid = jnp.concatenate([valid] * (plan.width // LANES), axis=1)
        part = acc[slot * rows - low : slot * rows - low + rows]
        pieces = []
        for start, off in zip(plan.start, plan.off):
            inside = (lane >= off) & (lane < off + plan.half)
            block = part[:, start : start + plan.width]
            pieces.append(jnp.where(inside, block * valid, valid).astype(jnp.bfloat16))
        at = slice(slot * rows, slot * rows + rows)
        own_ref[at, :] = jnp.where(first, pieces[0], pieces[1])
        other_ref[at, :] = jnp.where(first, pieces[1], pieces[0])


def group_of(live_ref):
    slots, rows = live_ref.shape
    return rows * (2 if slots % 2 == 0 else 1)


def project_kernel(
    plan,
    layer,
    count_ref,
    feats_hbm,
    weights_hbm,
    mask_hbm,
    own_ref,
    other_ref,
    feats_ref,
    weights_ref,
    mask_ref,
    live_ref,
    sems,
):
    size = group_of(live_ref)
    groups = feats_ref.shape[0] // size
    copies = [
        pltpu.make_async_copy(mask_hbm, mask_ref, sems.at[groups + 1]),
        pltpu.make_async_copy(weights_hbm.at[layer], weights_ref, sems.at[groups]),
    ]
    for index in range(groups):
        at = pl.ds(index * size, size)
        copies.append(
            pltpu.make_async_copy(feats_hbm.at[at], feats_ref.at[at], sems.at[index])
        )
    for copy in copies:
        copy.start()
    copies[0].wait()
    marks = mask_ref[...].astype(jnp.float32)
    slot_ids = lax.broadcasted_iota(jnp.int32, marks.shape, 0)
    live_ref[...] = jnp.where(slot_ids < count_ref[0], marks, 0.0)
    copies[1].wait()
    for index in range(groups):
        copies[2 + index].wait()
        low = index * size
        project_rows(plan, live_ref, feats_ref, weights_ref, own_ref, other_ref, low, low + size)


def attend(plan, query, scale_ref, own_ref, recv_ref, chunk_refs, mix):
    me_t, _, side = place()
    first = side == 0
    off = jnp.where(first, plan.off[0], plan.off[1])
    pad = jnp.where(first, plan.half if plan.off[0] == 0 else 0, plan.half if plan.off[1] == 0 else 0)
    lane = lax.broadcasted_iota(jnp.int32, (1, plan.width), 1)
    factor = SOFT_CAP * math.log2(math.e)
    n_keys = own_ref.shape[0]
    block = min(n_keys, 512)
    masked, scales = [], []
    for head in range(plan.heads):
        low = off + head * plan.head_dim
        masked.append(
            jnp.where((lane >= low) & (lane < low + plan.head_dim), query, jnp.zeros_like(query))
        )
        scales.append(
            scale_ref[side * plan.heads + head] * (1.0 / (SOFT_CAP * math.sqrt(plan.head_dim)))
        )
    stacked = jnp.concatenate(masked, axis=0)
    for at in range(0, n_keys, block):
        mine = own_ref[at : at + block, :]
        theirs = recv_ref[at : at + block, :]
        keys = jnp.where(first, mine, theirs)
        values = jnp.where(first, theirs, mine)
        scores = lax.dot_general(
            stacked, keys, (((1,), (1,)), ((), ())), preferred_element_type=jnp.float32
        )
        weights = []
        for head, scale in enumerate(scales):
            part = scores[head * plan.n_q : head * plan.n_q + plan.n_q]
            weights.append(jnp.exp2(jnp.tanh(part * scale) * factor).astype(jnp.bfloat16))
        part = jnp.dot(
            jnp.concatenate(weights, axis=0), values, preferred_element_type=jnp.float32
        )
        mix[...] = part if at == 0 else mix[...] + part
    totals = [mix[head * plan.n_q : head * plan.n_q + plan.n_q, :] for head in range(plan.heads)]
    result = jnp.zeros((plan.n_q, plan.width), jnp.float32)
    spot = lane - pad
    spare = (spot >= 0) & (spot < 2 * SPLIT)
    for head in range(plan.heads):
        low = off + head * plan.head_dim
        keep = (lane >= low) & (lane < low + plan.head_dim)
        keep = keep | (spare & (jnp.bitwise_and(spot, SPLIT - 1) == head))
        result = jnp.where(keep, totals[head], result)
    rounded = result.astype(jnp.bfloat16).astype(jnp.float32)
    late = spare & (spot >= SPLIT)
    mix[: plan.n_q, :] = jnp.where(late, result - rounded, rounded)
    for index, ref in enumerate(chunk_refs):
        rows = plan.n_q // plan.n_t
        ref[...] = mix[rows_at(jnp.bitwise_xor(me_t, index), rows), :].astype(ref.dtype)


def query_of(plan, states, gain, wq, wq_pad):
    side = lax.axis_index("kv")
    mean = jnp.mean(states * states, axis=-1, keepdims=True)
    normed = (states * lax.rsqrt(mean + NORM_EPS) * gain).astype(jnp.bfloat16)
    wq_pad[...] = jnp.zeros_like(wq_pad)
    step = max(plan.off)
    wq_pad[pl.ds(pl.multiple_of(side * step, step), plan.half), :] = wq
    return lax.dot_general(
        normed, wq_pad[...], (((1,), (1,)), ((), ())), preferred_element_type=jnp.float32
    ).astype(jnp.bfloat16)


def gather_queries(plan, refs, states_ref):
    _, me_h, me_k = place()
    for dh in range(plan.n_h):
        for dk in range(plan.n_k):
            index = jnp.bitwise_xor(me_h, dh) * plan.n_k + jnp.bitwise_xor(me_k, dk)
            block = refs[dh * plan.n_k + dk][...]
            states_ref[rows_at(index, plan.q_rows), :] = block.astype(jnp.float32)


def first_kernel(
    plan, scale_ref, q_ref, qk_ref, qx_ref, qxk_ref, gain_ref, wq_ref, own_ref, recv_ref, *rest
):
    chunks, (states_ref, wq_pad, mix) = rest[: plan.n_t], rest[plan.n_t :]
    gather_queries(plan, (q_ref, qk_ref, qx_ref, qxk_ref), states_ref)
    query = query_of(plan, states_ref[...], gain_ref[0:1, :], wq_ref[0], wq_pad)
    attend(plan, query, scale_ref, own_ref, recv_ref, chunks, mix)


def fill_out(plan, layer, wo_refs, wo_all):
    me_k = lax.axis_index("kv")
    for dh in range(plan.n_h):
        for dk in range(plan.n_k):
            index = dh * plan.n_k + jnp.bitwise_xor(me_k, dk)
            wo_all[rows_at(index, plan.half), :] = wo_refs[dh * plan.n_k + dk][layer]


def layer_kernel(
    plan,
    layer,
    scale_ref,
    q_ref,
    qk_ref,
    qx_ref,
    qxk_ref,
    block_ref,
    near_ref,
    far_ref,
    wo0,
    wo1,
    wo2,
    wo3,
    gain_ref,
    wq_ref,
    own_ref,
    recv_ref,
    *rest,
):
    chunks, rest = rest[: plan.n_t], rest[plan.n_t :]
    kept_ref, att, wo_all, states_ref, wq_pad, mix = rest
    me_t, me_h, me_k = place()
    rows = plan.n_q // plan.n_t
    fill_out(plan, layer - 1, (wo0, wo1, wo2, wo3), wo_all)
    for index, pair in enumerate(plan.rounds):
        for ref, flip in ((near_ref, 0), (far_ref, 1)):
            choice = [pair[k ^ flip] or (0, 0) for k in range(2)]
            dt = jnp.where(me_k == 0, choice[0][0], choice[1][0])
            dh = jnp.where(me_k == 0, choice[0][1], choice[1][1])
            att[rows_at(jnp.bitwise_xor(me_t, dt), rows), rows_at(dh, plan.cols)] = ref[
                index * rows : index * rows + rows, :
            ]
    att[rows_at(me_t, rows), : plan.cols] = block_ref[...]
    out = jnp.dot(att[...], wo_all[...], preferred_element_type=jnp.float32)
    gather_queries(plan, (q_ref, qk_ref, qx_ref, qxk_ref), states_ref)
    states = states_ref[...] + out
    states_ref[...] = states
    kept_ref[...] = states_ref[rows_at(me_h * plan.n_k + me_k, plan.q_rows), :]
    query = query_of(plan, states, gain_ref[layer : layer + 1, :], wq_ref[layer], wq_pad)
    attend(plan, query, scale_ref, own_ref, recv_ref, chunks, mix)


def last_kernel(plan, layer, kept_ref, near_ref, far_ref, wo0, wo1, wo2, wo3, out_ref, att, wo_all):
    me_t = lax.axis_index("tiles")
    fill_out(plan, layer, (wo0, wo1, wo2, wo3), wo_all)
    for index, ref in enumerate((near_ref, far_ref)):
        att[:, rows_at((me_t // plan.n_k + index) % plan.n_h, plan.cols)] = ref[...]
    out = jnp.dot(att[...], wo_all[...], preferred_element_type=jnp.float32)
    out_ref[...] = kept_ref[...] + out


def combine_kernel(plan, *refs):
    *parts, out_ref = refs
    side = lax.axis_index("kv")
    first = side == 0
    off = jnp.where(first, plan.off[0], plan.off[1])
    pad = jnp.where(first, plan.half if plan.off[0] == 0 else 0, plan.half if plan.off[1] == 0 else 0)
    lane = lax.broadcasted_iota(jnp.int32, (1, plan.width), 1)
    spot = lane - pad
    spare = (spot >= 0) & (spot < 2 * SPLIT)
    total = sum(ref[...].astype(jnp.float32) for ref in parts)
    below = jnp.ones_like(total)
    for head in range(plan.heads):
        low = off + head * plan.head_dim
        mine = spare & (jnp.bitwise_and(spot, SPLIT - 1) == head)
        weight = jnp.sum(jnp.where(mine, total, 0.0), axis=1, keepdims=True)
        below = jnp.where((lane >= low) & (lane < low + plan.head_dim), weight, below)
    out_ref[...] = (total / below).astype(jnp.bfloat16)


def vmem_call(kernel, out_shape, scalars, arrays, scratch, flops, far=(), sems=0):
    specs = [pl.BlockSpec(memory_space=pltpu.SMEM)] * len(scalars)
    specs += [pl.BlockSpec(memory_space=pltpu.VMEM)] * len(arrays)
    specs += [pl.BlockSpec(memory_space=pltpu.HBM)] * len(far)
    held = [*arrays, *jax.tree.leaves(out_shape), *scratch]
    scratch = scratch + ([pltpu.SemaphoreType.DMA((sems,))] if sems else [])
    grant = sum(math.prod(a.shape) * jnp.dtype(a.dtype).itemsize for a in held) + ROOM
    return pl.pallas_call(
        kernel,
        out_shape=out_shape,
        in_specs=specs,
        out_specs=[pl.BlockSpec(memory_space=pltpu.VMEM) for _ in out_shape]
        if isinstance(out_shape, list)
        else pl.BlockSpec(memory_space=pltpu.VMEM),
        scratch_shapes=scratch,
        cost_estimate=pl.CostEstimate(flops=flops, bytes_accessed=1 << 20, transcendentals=0),
        compiler_params=pltpu.CompilerParams(vmem_limit_bytes=grant),
    )(*scalars, *arrays, *far)


def fast_body(plan, features, counts, tile_mask, queries, norm_gain, head_scale, w_query, w_kv, w_out):
    layer_count = w_kv.shape[0]
    rows = plan.n_q // plan.n_t
    axes = ("tiles", "heads", "kv")
    devices = [
        (t, h, k) for t in range(plan.n_t) for h in range(plan.n_h) for k in range(plan.n_k)
    ]
    side = lax.axis_index("kv")

    def number(t, h, k):
        return (t * plan.n_h + h) * plan.n_k + k

    def swap(value, axis):
        size = {"heads": plan.n_h, "kv": plan.n_k}[axis]
        return lax.ppermute(value, axis, [(i, i ^ 1) for i in range(size)])

    def exchange(chunks):
        received = []
        for d in range(plan.n_t - 1, 0, -1):
            received.append(lax.ppermute(chunks[d], "tiles", [(i, i ^ d) for i in range(plan.n_t)]))
        shape = jax.ShapeDtypeStruct((rows, plan.width), jnp.bfloat16)
        attended = vmem_call(
            functools.partial(combine_kernel, plan), shape, [], [chunks[0], *received], [], 1 << 20
        )
        partner = swap(attended, "kv")
        low = jnp.where(side == 0, attended, partner)
        high = jnp.where(side == 0, partner, attended)
        lead = plan.start[1]
        overlap = jnp.where(
            lax.broadcasted_iota(jnp.int32, (1, plan.width - lead), 1) < plan.half - lead,
            low[:, lead:],
            high[:, : plan.width - lead],
        )
        return jnp.concatenate([low[:, :lead], overlap, high[:, plan.width - lead :]], axis=1)

    def spread(block):
        received = []
        for pair in plan.rounds:
            links = [
                (number(t, h, k), number(t ^ pair[k][0], h ^ pair[k][1], k))
                for t, h, k in devices
                if pair[k] is not None
            ]
            received.append(lax.ppermute(block, axes, links))
        near = jnp.concatenate(received, axis=0)
        return near, swap(near, "kv")

    def collect(block):
        received = []
        for turn in range(plan.n_h):
            links = []
            for t, h, k in devices:
                source_t = h * plan.n_k + k
                source_h = h ^ ((turn + t // plan.n_k) % plan.n_h)
                source_k = plan.n_k - 1 - t % plan.n_k
                links.append((number(source_t, source_h, source_k), number(t, h, k)))
            received.append(lax.ppermute(block, axes, links))
        return received

    weights = w_kv.reshape(layer_count, w_kv.shape[1], plan.cols)
    wq = jnp.swapaxes(w_query, 1, 2)
    q_x = swap(queries, "heads")
    q_k = swap(queries, "kv")
    q_xk = swap(q_x, "kv")
    wo_x = swap(w_out, "heads")
    wo = [w_out, swap(w_out, "kv"), wo_x, swap(wo_x, "kv")]
    tiles = features.shape[0]
    bf16, f32 = jnp.bfloat16, jnp.float32
    feat = features.shape[1]
    piece = jax.ShapeDtypeStruct((tiles, plan.width), bf16)
    cost = 2 * tiles * feat * plan.cols
    streamed = [
        pltpu.with_memory_space_constraint(a, pltpu.HBM) for a in (features, weights, tile_mask)
    ]
    pairs = []
    for layer in range(layer_count):
        own, other = vmem_call(
            functools.partial(project_kernel, plan, layer),
            [piece, piece],
            [counts],
            [],
            [
                pltpu.VMEM((tiles, feat), bf16),
                pltpu.VMEM((feat, plan.cols), bf16),
                pltpu.VMEM(tile_mask.shape, jnp.int32),
                pltpu.VMEM(tile_mask.shape, f32),
            ],
            cost,
            streamed,
            tile_mask.shape[0] + 2,
        )
        pairs.append((own, swap(other, "kv")))

    chunk_shapes = [jax.ShapeDtypeStruct((rows, plan.width), f32)]
    chunk_shapes += [jax.ShapeDtypeStruct((rows, plan.width), bf16)] * (plan.n_t - 1)
    wq_scratch = pltpu.VMEM((plan.width, plan.dq), bf16)
    states_scratch = pltpu.VMEM((plan.n_q, plan.dq), f32)
    mix_scratch = pltpu.VMEM((plan.heads * plan.n_q, plan.width), f32)
    wo_scratch = pltpu.VMEM((plan.n_h * plan.cols, plan.dq), bf16)

    work = 4 * plan.n_q * tiles * plan.width
    chunks = vmem_call(
        functools.partial(first_kernel, plan),
        chunk_shapes,
        [head_scale],
        [queries, q_k, q_x, q_xk, norm_gain, wq, *pairs[0]],
        [states_scratch, wq_scratch, mix_scratch],
        work,
    )
    block = exchange(chunks)
    near, far = spread(block)
    outs = vmem_call(
        functools.partial(layer_kernel, plan, 1),
        chunk_shapes + [jax.ShapeDtypeStruct((plan.q_rows, plan.dq), f32)],
        [head_scale],
        [queries, q_k, q_x, q_xk, block, near, far, *wo, norm_gain, wq]
        + [pltpu.with_memory_space_constraint(a, pltpu.VMEM) for a in pairs[1]],
        [
            pltpu.VMEM((plan.n_q, plan.n_h * plan.cols), bf16),
            wo_scratch,
            states_scratch,
            wq_scratch,
            mix_scratch,
        ],
        work,
    )
    chunks, kept = outs[: plan.n_t], outs[plan.n_t]
    block = exchange(chunks)
    near, far = collect(block)
    return vmem_call(
        functools.partial(last_kernel, plan, 1),
        jax.ShapeDtypeStruct((plan.q_rows, plan.dq), f32),
        [],
        [kept, near, far, *wo],
        [pltpu.VMEM((plan.q_rows, plan.n_h * plan.cols), bf16), wo_scratch],
        2 * plan.q_rows * plan.dq * plan.dq,
    )


def solution(mesh):
    def body(features, counts, tile_mask, queries, norm_gain, head_scale, w_query, w_kv, w_out):
        args = (features, counts, tile_mask, queries, norm_gain, head_scale, w_query, w_kv, w_out)
        plan = Plan(mesh, queries, head_scale, w_kv)
        if w_kv.shape[0] == 2 and plan.usable():
            return fast_body(plan, *args)
        return generic_body(*args)

    return jax.shard_map(
        body,
        mesh=mesh,
        in_specs=(
            P(("groups", "tiles"), None),
            P(("groups", "tiles")),
            P(("groups", "tiles"), None),
            P(("heads", "kv"), None),
            P(),
            P("heads"),
            P(None, None, ("heads", "kv")),
            P(None, None, "kv", "heads"),
            P(None, ("heads", "kv"), None),
        ),
        out_specs=P(("groups", "heads", "kv"), None),
        check_vma=False,
    )
```

```python
import functools
import math

import jax
import jax.numpy as jnp
from jax import lax
from jax.experimental import pallas as pl
from jax.experimental.pallas import tpu as pltpu
from jax.sharding import PartitionSpec as P


SOFT_CAP = 50.0
NORM_EPS = 1e-06
LANES = 128
SPLIT = 16
ROOM = 4 << 20


def normalize(hidden, gain_row):
    return (
        hidden * lax.rsqrt(jnp.mean(hidden * hidden, axis=-1, keepdims=True) + NORM_EPS) * gain_row
    )


def generic_body(features, counts, tile_mask, queries, norm_gain, head_scale, w_query, w_kv, w_out):
    slot_count = tile_mask.shape[0]
    block_rows = tile_mask.shape[1]
    total_rows = slot_count * block_rows
    half_rows = total_rows // 2
    layer_count = w_kv.shape[0]
    head_cols = w_kv.shape[3]
    heads_local = head_scale.shape[0]
    head_dim = head_cols // heads_local
    kv_side = lax.axis_index("kv")
    kv_weights = w_kv[:, :, 0, :]
    slot_ids = jnp.arange(slot_count, dtype=jnp.int32)

    def add_block(slot_at, current):
        block_feats = lax.dynamic_slice_in_dim(features, slot_at * block_rows, block_rows, 0)
        result = jnp.einsum(
            "rf,lfc->lrc", block_feats, kv_weights, preferred_element_type=jnp.float32
        )
        return lax.dynamic_update_slice_in_dim(
            current, result.astype(jnp.bfloat16), slot_at * block_rows, 1
        )

    own_count = counts[0]
    projected = jnp.zeros((layer_count, total_rows, head_cols), jnp.bfloat16)
    projected = lax.fori_loop(jnp.int32(0), own_count, add_block, projected)
    live_mask = tile_mask * (slot_ids < own_count).astype(jnp.int32)[:, None]
    kv_local = lax.all_to_all(projected, "kv", split_axis=1, concat_axis=2, tiled=True)
    valid_tiles = lax.dynamic_slice_in_dim(
        live_mask.reshape(total_rows).astype(jnp.float32), kv_side * half_rows, half_rows, 0
    )
    states = queries.astype(jnp.float32)
    scale_vec = head_scale / math.sqrt(head_dim)
    for layer_at in range(layer_count):
        normed = lax.all_gather(
            normalize(states, norm_gain[layer_at]).astype(jnp.bfloat16),
            ("heads", "kv"),
            axis=0,
            tiled=True,
        )
        query_part = jnp.dot(normed, w_query[layer_at], preferred_element_type=jnp.float32).astype(
            jnp.bfloat16
        )
        query_cols = lax.all_gather(query_part, "kv", axis=1, tiled=True)
        n_queries = query_cols.shape[0]
        query_heads = query_cols.reshape(n_queries, heads_local, head_dim)
        key_heads = kv_local[layer_at, :, :head_cols].reshape(half_rows, heads_local, head_dim)
        value_heads = kv_local[layer_at, :, head_cols:].reshape(half_rows, heads_local, head_dim)
        scores = jnp.einsum(
            "qhd,khd->hqk", query_heads, key_heads, preferred_element_type=jnp.float32
        )
        scores = scores * scale_vec[:, None, None]
        capped = SOFT_CAP * jnp.tanh(scores / SOFT_CAP)
        weights_p = jnp.exp(capped) * valid_tiles[None, None, :]
        totals = jnp.sum(weights_p, axis=2)
        partial_value = jnp.einsum(
            "hqk,khd->qhd",
            weights_p.astype(jnp.bfloat16),
            value_heads,
            preferred_element_type=jnp.float32,
        )
        totals, partial_value = lax.psum((totals, partial_value), ("tiles", "kv"))
        attended = (
            (partial_value / jnp.transpose(totals)[:, :, None])
            .reshape(n_queries, head_cols)
            .astype(jnp.bfloat16)
        )
        own_cols = lax.dynamic_slice_in_dim(attended, kv_side * (head_cols // 2), head_cols // 2, 1)
        states = states + lax.psum_scatter(
            jnp.dot(own_cols, w_out[layer_at], preferred_element_type=jnp.float32),
            ("heads", "kv"),
            scatter_dimension=0,
            tiled=True,
        )
    return states


class Plan:
    def __init__(self, mesh, queries, head_scale, w_kv):
        self.n_t, self.n_h, self.n_k = (mesh.shape[a] for a in ("tiles", "heads", "kv"))
        self.q_rows, self.dq = queries.shape
        self.n_q = self.q_rows * self.n_h * self.n_k
        self.cols = w_kv.shape[3]
        self.heads = head_scale.shape[0] // self.n_k
        self.head_dim = self.cols // head_scale.shape[0]
        self.half = self.heads * self.head_dim
        self.width = -(-self.half // LANES) * LANES
        self.start = [k * self.half // LANES * LANES for k in range(self.n_k)]
        self.off = [k * self.half - s for k, s in enumerate(self.start)]
        steps = [1, *range(self.n_t - 1, 1, -1)]
        self.rounds = [
            tuple((step, (k + index) % 2) for k in range(self.n_k))
            for index, step in enumerate(steps)
        ]
        self.rounds.append((None,) * (self.n_k - 1) + ((0, 1),))

    def usable(self):
        return (
            self.n_k == 2
            and self.n_h == 2
            and self.n_t == self.n_h * self.n_k
            and self.half * self.n_k == self.cols
            and self.cols % LANES == 0
            and self.q_rows % 16 == 0
            and self.off[0] == 0
            and all(s + self.width <= self.cols for s in self.start)
            and all(o == 0 or o + self.half == self.width for o in self.off)
            and self.width - self.half >= 2 * SPLIT
            and self.heads <= SPLIT
        )


def place():
    return lax.axis_index("tiles"), lax.axis_index("heads"), lax.axis_index("kv")


def rows_at(index, size):
    return pl.ds(pl.multiple_of(index * size, size), size)


def project_rows(plan, live_ref, feats, weights, own_ref, other_ref, low, high):
    first = lax.axis_index("kv") == 0
    rows = live_ref.shape[1]
    lane = lax.broadcasted_iota(jnp.int32, (1, plan.width), 1)
    acc = jnp.dot(feats[low:high, :], weights[...], preferred_element_type=jnp.float32)
    for slot in range(low // rows, high // rows):
        valid = jnp.broadcast_to(live_ref[slot : slot + 1, :], (LANES, rows)).T
        valid = jnp.concatenate([valid] * (plan.width // LANES), axis=1)
        part = acc[slot * rows - low : slot * rows - low + rows]
        pieces = []
        for start, off in zip(plan.start, plan.off):
            inside = (lane >= off) & (lane < off + plan.half)
            block = part[:, start : start + plan.width]
            pieces.append(jnp.where(inside, block * valid, valid).astype(jnp.bfloat16))
        at = slice(slot * rows, slot * rows + rows)
        own_ref[at, :] = jnp.where(first, pieces[0], pieces[1])
        other_ref[at, :] = jnp.where(first, pieces[1], pieces[0])


def group_of(live_ref):
    slots, rows = live_ref.shape
    return rows * (2 if slots % 2 == 0 else 1)


def project_kernel(
    plan,
    layer,
    count_ref,
    feats_hbm,
    weights_hbm,
    mask_hbm,
    own_ref,
    other_ref,
    feats_ref,
    weights_ref,
    mask_ref,
    live_ref,
    sems,
):
    size = group_of(live_ref)
    bounds = sorted({0, size, feats_ref.shape[0]})
    groups = len(bounds) - 1
    copies = [
        pltpu.make_async_copy(mask_hbm, mask_ref, sems.at[groups + 1]),
        pltpu.make_async_copy(weights_hbm.at[layer], weights_ref, sems.at[groups]),
    ]
    for index in range(groups):
        at = pl.ds(bounds[index], bounds[index + 1] - bounds[index])
        copies.append(
            pltpu.make_async_copy(feats_hbm.at[at], feats_ref.at[at], sems.at[index])
        )
    for copy in copies:
        copy.start()
    copies[0].wait()
    marks = mask_ref[...].astype(jnp.float32)
    slot_ids = lax.broadcasted_iota(jnp.int32, marks.shape, 0)
    live_ref[...] = jnp.where(slot_ids < count_ref[0], marks, 0.0)
    copies[1].wait()
    for index in range(groups):
        copies[2 + index].wait()
        low, high = bounds[index], bounds[index + 1]
        project_rows(plan, live_ref, feats_ref, weights_ref, own_ref, other_ref, low, high)


def attend(plan, query, scale_ref, own_ref, recv_ref, chunk_refs, mix):
    me_t, _, side = place()
    first = side == 0
    off = jnp.where(first, plan.off[0], plan.off[1])
    pad = jnp.where(first, plan.half if plan.off[0] == 0 else 0, plan.half if plan.off[1] == 0 else 0)
    lane = lax.broadcasted_iota(jnp.int32, (1, plan.width), 1)
    factor = SOFT_CAP * math.log2(math.e)
    n_keys = own_ref.shape[0]
    block = min(n_keys, 512)
    masked, scales = [], []
    for head in range(plan.heads):
        low = off + head * plan.head_dim
        masked.append(
            jnp.where((lane >= low) & (lane < low + plan.head_dim), query, jnp.zeros_like(query))
        )
        scales.append(
            scale_ref[side * plan.heads + head] * (1.0 / (SOFT_CAP * math.sqrt(plan.head_dim)))
        )
    stacked = jnp.concatenate(masked, axis=0)
    for at in range(0, n_keys, block):
        mine = own_ref[at : at + block, :]
        theirs = recv_ref[at : at + block, :]
        keys = jnp.where(first, mine, theirs)
        values = jnp.where(first, theirs, mine)
        scores = lax.dot_general(
            stacked, keys, (((1,), (1,)), ((), ())), preferred_element_type=jnp.float32
        )
        weights = []
        for head, scale in enumerate(scales):
            part = scores[head * plan.n_q : head * plan.n_q + plan.n_q]
            weights.append(jnp.exp2(jnp.tanh(part * scale) * factor).astype(jnp.bfloat16))
        part = jnp.dot(
            jnp.concatenate(weights, axis=0), values, preferred_element_type=jnp.float32
        )
        mix[...] = part if at == 0 else mix[...] + part
    totals = [mix[head * plan.n_q : head * plan.n_q + plan.n_q, :] for head in range(plan.heads)]
    result = jnp.zeros((plan.n_q, plan.width), jnp.float32)
    spot = lane - pad
    spare = (spot >= 0) & (spot < 2 * SPLIT)
    for head in range(plan.heads):
        low = off + head * plan.head_dim
        keep = (lane >= low) & (lane < low + plan.head_dim)
        keep = keep | (spare & (jnp.bitwise_and(spot, SPLIT - 1) == head))
        result = jnp.where(keep, totals[head], result)
    rounded = result.astype(jnp.bfloat16).astype(jnp.float32)
    late = spare & (spot >= SPLIT)
    mix[: plan.n_q, :] = jnp.where(late, result - rounded, rounded)
    for index, ref in enumerate(chunk_refs):
        rows = plan.n_q // plan.n_t
        ref[...] = mix[rows_at(jnp.bitwise_xor(me_t, index), rows), :].astype(ref.dtype)


def query_of(plan, states, gain, wq, wq_pad):
    side = lax.axis_index("kv")
    mean = jnp.mean(states * states, axis=-1, keepdims=True)
    normed = (states * lax.rsqrt(mean + NORM_EPS) * gain).astype(jnp.bfloat16)
    wq_pad[...] = jnp.zeros_like(wq_pad)
    step = max(plan.off)
    wq_pad[pl.ds(pl.multiple_of(side * step, step), plan.half), :] = wq
    return lax.dot_general(
        normed, wq_pad[...], (((1,), (1,)), ((), ())), preferred_element_type=jnp.float32
    ).astype(jnp.bfloat16)


def gather_queries(plan, refs, states_ref):
    _, me_h, me_k = place()
    for dh in range(plan.n_h):
        for dk in range(plan.n_k):
            index = jnp.bitwise_xor(me_h, dh) * plan.n_k + jnp.bitwise_xor(me_k, dk)
            block = refs[dh * plan.n_k + dk][...]
            states_ref[rows_at(index, plan.q_rows), :] = block.astype(jnp.float32)


def first_kernel(
    plan, scale_ref, q_ref, qk_ref, qx_ref, qxk_ref, gain_ref, wq_ref, own_ref, recv_ref, *rest
):
    chunks, (states_ref, wq_pad, mix) = rest[: plan.n_t], rest[plan.n_t :]
    gather_queries(plan, (q_ref, qk_ref, qx_ref, qxk_ref), states_ref)
    query = query_of(plan, states_ref[...], gain_ref[0:1, :], wq_ref[0], wq_pad)
    attend(plan, query, scale_ref, own_ref, recv_ref, chunks, mix)


def fill_out(plan, layer, wo_refs, wo_all):
    me_k = lax.axis_index("kv")
    for dh in range(plan.n_h):
        for dk in range(plan.n_k):
            index = dh * plan.n_k + jnp.bitwise_xor(me_k, dk)
            wo_all[rows_at(index, plan.half), :] = wo_refs[dh * plan.n_k + dk][layer]


def layer_kernel(
    plan,
    layer,
    scale_ref,
    q_ref,
    qk_ref,
    qx_ref,
    qxk_ref,
    block_ref,
    near_ref,
    far_ref,
    wo0,
    wo1,
    wo2,
    wo3,
    gain_ref,
    wq_ref,
    own_ref,
    recv_ref,
    *rest,
):
    chunks, rest = rest[: plan.n_t], rest[plan.n_t :]
    kept_ref, att, wo_all, states_ref, wq_pad, mix = rest
    me_t, me_h, me_k = place()
    rows = plan.n_q // plan.n_t
    fill_out(plan, layer - 1, (wo0, wo1, wo2, wo3), wo_all)
    for index, pair in enumerate(plan.rounds):
        for ref, flip in ((near_ref, 0), (far_ref, 1)):
            choice = [pair[k ^ flip] or (0, 0) for k in range(2)]
            dt = jnp.where(me_k == 0, choice[0][0], choice[1][0])
            dh = jnp.where(me_k == 0, choice[0][1], choice[1][1])
            att[rows_at(jnp.bitwise_xor(me_t, dt), rows), rows_at(dh, plan.cols)] = ref[
                index * rows : index * rows + rows, :
            ]
    att[rows_at(me_t, rows), : plan.cols] = block_ref[...]
    out = jnp.dot(att[...], wo_all[...], preferred_element_type=jnp.float32)
    gather_queries(plan, (q_ref, qk_ref, qx_ref, qxk_ref), states_ref)
    states = states_ref[...] + out
    states_ref[...] = states
    kept_ref[...] = states_ref[rows_at(me_h * plan.n_k + me_k, plan.q_rows), :]
    query = query_of(plan, states, gain_ref[layer : layer + 1, :], wq_ref[layer], wq_pad)
    attend(plan, query, scale_ref, own_ref, recv_ref, chunks, mix)


def last_kernel(plan, layer, kept_ref, near_ref, far_ref, wo0, wo1, wo2, wo3, out_ref, att, wo_all):
    me_t = lax.axis_index("tiles")
    fill_out(plan, layer, (wo0, wo1, wo2, wo3), wo_all)
    for index, ref in enumerate((near_ref, far_ref)):
        att[:, rows_at((me_t // plan.n_k + index) % plan.n_h, plan.cols)] = ref[...]
    out = jnp.dot(att[...], wo_all[...], preferred_element_type=jnp.float32)
    out_ref[...] = kept_ref[...] + out


def combine_kernel(plan, *refs):
    *parts, out_ref = refs
    side = lax.axis_index("kv")
    first = side == 0
    off = jnp.where(first, plan.off[0], plan.off[1])
    pad = jnp.where(first, plan.half if plan.off[0] == 0 else 0, plan.half if plan.off[1] == 0 else 0)
    lane = lax.broadcasted_iota(jnp.int32, (1, plan.width), 1)
    spot = lane - pad
    spare = (spot >= 0) & (spot < 2 * SPLIT)
    total = sum(ref[...].astype(jnp.float32) for ref in parts)
    below = jnp.ones_like(total)
    for head in range(plan.heads):
        low = off + head * plan.head_dim
        mine = spare & (jnp.bitwise_and(spot, SPLIT - 1) == head)
        weight = jnp.sum(jnp.where(mine, total, 0.0), axis=1, keepdims=True)
        below = jnp.where((lane >= low) & (lane < low + plan.head_dim), weight, below)
    out_ref[...] = (total / below).astype(jnp.bfloat16)


def vmem_call(kernel, out_shape, scalars, arrays, scratch, flops, far=(), sems=0):
    specs = [pl.BlockSpec(memory_space=pltpu.SMEM)] * len(scalars)
    specs += [pl.BlockSpec(memory_space=pltpu.VMEM)] * len(arrays)
    specs += [pl.BlockSpec(memory_space=pltpu.HBM)] * len(far)
    held = [*arrays, *jax.tree.leaves(out_shape), *scratch]
    scratch = scratch + ([pltpu.SemaphoreType.DMA((sems,))] if sems else [])
    grant = sum(math.prod(a.shape) * jnp.dtype(a.dtype).itemsize for a in held) + ROOM
    return pl.pallas_call(
        kernel,
        out_shape=out_shape,
        in_specs=specs,
        out_specs=[pl.BlockSpec(memory_space=pltpu.VMEM) for _ in out_shape]
        if isinstance(out_shape, list)
        else pl.BlockSpec(memory_space=pltpu.VMEM),
        scratch_shapes=scratch,
        cost_estimate=pl.CostEstimate(flops=flops, bytes_accessed=1 << 20, transcendentals=0),
        compiler_params=pltpu.CompilerParams(vmem_limit_bytes=grant),
    )(*scalars, *arrays, *far)


def fast_body(plan, features, counts, tile_mask, queries, norm_gain, head_scale, w_query, w_kv, w_out):
    layer_count = w_kv.shape[0]
    rows = plan.n_q // plan.n_t
    axes = ("tiles", "heads", "kv")
    devices = [
        (t, h, k) for t in range(plan.n_t) for h in range(plan.n_h) for k in range(plan.n_k)
    ]
    side = lax.axis_index("kv")

    def number(t, h, k):
        return (t * plan.n_h + h) * plan.n_k + k

    def swap(value, axis):
        size = {"heads": plan.n_h, "kv": plan.n_k}[axis]
        return lax.ppermute(value, axis, [(i, i ^ 1) for i in range(size)])

    def exchange(chunks):
        received = []
        for d in range(plan.n_t - 1, 0, -1):
            received.append(lax.ppermute(chunks[d], "tiles", [(i, i ^ d) for i in range(plan.n_t)]))
        shape = jax.ShapeDtypeStruct((rows, plan.width), jnp.bfloat16)
        attended = vmem_call(
            functools.partial(combine_kernel, plan), shape, [], [chunks[0], *received], [], 1 << 20
        )
        partner = swap(attended, "kv")
        low = jnp.where(side == 0, attended, partner)
        high = jnp.where(side == 0, partner, attended)
        lead = plan.start[1]
        overlap = jnp.where(
            lax.broadcasted_iota(jnp.int32, (1, plan.width - lead), 1) < plan.half - lead,
            low[:, lead:],
            high[:, : plan.width - lead],
        )
        return jnp.concatenate([low[:, :lead], overlap, high[:, plan.width - lead :]], axis=1)

    def spread(block):
        received = []
        for pair in plan.rounds:
            links = [
                (number(t, h, k), number(t ^ pair[k][0], h ^ pair[k][1], k))
                for t, h, k in devices
                if pair[k] is not None
            ]
            received.append(lax.ppermute(block, axes, links))
        near = jnp.concatenate(received, axis=0)
        return near, swap(near, "kv")

    def collect(block):
        received = []
        for turn in range(plan.n_h):
            links = []
            for t, h, k in devices:
                source_t = h * plan.n_k + k
                source_h = h ^ ((turn + t // plan.n_k) % plan.n_h)
                source_k = plan.n_k - 1 - t % plan.n_k
                links.append((number(source_t, source_h, source_k), number(t, h, k)))
            received.append(lax.ppermute(block, axes, links))
        return received

    weights = w_kv.reshape(layer_count, w_kv.shape[1], plan.cols)
    wq = jnp.swapaxes(w_query, 1, 2)
    q_x = swap(queries, "heads")
    q_k = swap(queries, "kv")
    q_xk = swap(q_x, "kv")
    wo_x = swap(w_out, "heads")
    wo = [w_out, swap(w_out, "kv"), wo_x, swap(wo_x, "kv")]
    tiles = features.shape[0]
    bf16, f32 = jnp.bfloat16, jnp.float32
    feat = features.shape[1]
    piece = jax.ShapeDtypeStruct((tiles, plan.width), bf16)
    cost = 2 * tiles * feat * plan.cols
    streamed = [
        pltpu.with_memory_space_constraint(a, pltpu.HBM) for a in (features, weights, tile_mask)
    ]
    pairs = []
    for layer in range(layer_count):
        own, other = vmem_call(
            functools.partial(project_kernel, plan, layer),
            [piece, piece],
            [counts],
            [],
            [
                pltpu.VMEM((tiles, feat), bf16),
                pltpu.VMEM((feat, plan.cols), bf16),
                pltpu.VMEM(tile_mask.shape, jnp.int32),
                pltpu.VMEM(tile_mask.shape, f32),
            ],
            cost,
            streamed,
            tile_mask.shape[0] + 2,
        )
        pairs.append((own, swap(other, "kv")))

    chunk_shapes = [jax.ShapeDtypeStruct((rows, plan.width), f32)]
    chunk_shapes += [jax.ShapeDtypeStruct((rows, plan.width), bf16)] * (plan.n_t - 1)
    wq_scratch = pltpu.VMEM((plan.width, plan.dq), bf16)
    states_scratch = pltpu.VMEM((plan.n_q, plan.dq), f32)
    mix_scratch = pltpu.VMEM((plan.heads * plan.n_q, plan.width), f32)
    wo_scratch = pltpu.VMEM((plan.n_h * plan.cols, plan.dq), bf16)

    work = 4 * plan.n_q * tiles * plan.width
    chunks = vmem_call(
        functools.partial(first_kernel, plan),
        chunk_shapes,
        [head_scale],
        [queries, q_k, q_x, q_xk, norm_gain, wq, *pairs[0]],
        [states_scratch, wq_scratch, mix_scratch],
        work,
    )
    block = exchange(chunks)
    near, far = spread(block)
    outs = vmem_call(
        functools.partial(layer_kernel, plan, 1),
        chunk_shapes + [jax.ShapeDtypeStruct((plan.q_rows, plan.dq), f32)],
        [head_scale],
        [queries, q_k, q_x, q_xk, block, near, far, *wo, norm_gain, wq]
        + [pltpu.with_memory_space_constraint(a, pltpu.VMEM) for a in pairs[1]],
        [
            pltpu.VMEM((plan.n_q, plan.n_h * plan.cols), bf16),
            wo_scratch,
            states_scratch,
            wq_scratch,
            mix_scratch,
        ],
        work,
    )
    chunks, kept = outs[: plan.n_t], outs[plan.n_t]
    block = exchange(chunks)
    near, far = collect(block)
    return vmem_call(
        functools.partial(last_kernel, plan, 1),
        jax.ShapeDtypeStruct((plan.q_rows, plan.dq), f32),
        [],
        [kept, near, far, *wo],
        [pltpu.VMEM((plan.q_rows, plan.n_h * plan.cols), bf16), wo_scratch],
        2 * plan.q_rows * plan.dq * plan.dq,
    )


def solution(mesh):
    def body(features, counts, tile_mask, queries, norm_gain, head_scale, w_query, w_kv, w_out):
        args = (features, counts, tile_mask, queries, norm_gain, head_scale, w_query, w_kv, w_out)
        plan = Plan(mesh, queries, head_scale, w_kv)
        if w_kv.shape[0] == 2 and plan.usable():
            return fast_body(plan, *args)
        return generic_body(*args)

    return jax.shard_map(
        body,
        mesh=mesh,
        in_specs=(
            P(("groups", "tiles"), None),
            P(("groups", "tiles")),
            P(("groups", "tiles"), None),
            P(("heads", "kv"), None),
            P(),
            P("heads"),
            P(None, None, ("heads", "kv")),
            P(None, None, "kv", "heads"),
            P(None, ("heads", "kv"), None),
        ),
        out_specs=P(("groups", "heads", "kv"), None),
        check_vma=False,
    )
```
